256 devices in a mesh: dp: 128 (over z, x, y), rep: 2 (over core).
Axes of the slice: x: 4, y: 4, z: 8, core: 2. Of those that a mesh axis runs over, the one named last changes fastest.
Arguments:
- queries: bfloat16 [196608, 256], P(('dp', 'rep')), may hold values from -100 to 100
- candidates: bfloat16 [196608, 256], P(('dp', 'rep')), may hold values from -6 to 6
- bucket: int32 [196608, 1], P(('dp', 'rep')), may hold values from 0 to 127, as said below
Outputs:
- query_loss: float32 [196608], P(('dp', 'rep'))
- bucket_loss: float32 [128], P('dp')
The draws below stay inside these ranges and needn't reach their ends.
Inputs may be any that keep to these rules, and one draw needn't show every extreme that they name: The 768 rows of one device name any bucket at most 12 times; on some device some bucket is named exactly 12 times; a bucket may be named by no row at all.
All inputs are finite; a program needn't handle non-finite values.
Results may differ from the reference program's by a relative error of at most 0.0003.
Values may be sent and summed in bfloat16 or wider, within the bound.
No kernel may reach another device: no remote copies, remote signals or barrier semaphores. Data moves between devices by JAX's collectives and lax.ppermute only.
A program may use at most 64 MiB of HBM per device.

```python
import jax
import jax.numpy as jnp
from jax import lax

E = 256
TOK_DEV = 768
CAP = 12
TOKENS = 196608
N_DP = 128
N_REP = 2


def shared_candidates(key):
    rows = jax.random.normal(jax.random.fold_in(key, 101), (TOKENS, E), jnp.float32)
    return jnp.clip(rows, -6.0, 6.0)


def draw_candidates(key, part):
    return shared_candidates(key).astype(jnp.bfloat16)


def draw_queries(key, part):
    base = jnp.clip(jax.random.normal(jax.random.fold_in(key, 202), (TOKENS, E), jnp.float32), -6.0, 6.0)
    return base.astype(jnp.bfloat16)


def draw_bucket(key, part):
    devices = TOKENS // TOK_DEV
    hot_count = max(1, N_DP // 32)
    order = jax.random.permutation(jax.random.fold_in(key, 11), N_DP).astype(jnp.int32)
    hot_rows = jnp.repeat(order[2:2 + hot_count], CAP)
    pool = jnp.repeat(order[2 + hot_count:], CAP)
    extra = TOK_DEV - hot_count * CAP

    def one_device(index):
        device_key = jax.random.fold_in(jax.random.fold_in(key, 23), index)
        picked = jax.random.permutation(device_key, pool)[:extra]
        rows = jnp.concatenate([hot_rows, picked], axis=0)
        return jax.random.permutation(jax.random.fold_in(device_key, 5), rows)
    blocks = jax.vmap(one_device)(jnp.arange(devices, dtype=jnp.int32))
    return blocks.reshape(TOKENS, 1).astype(jnp.int32)


def setup_inputs(seed: int = 0) -> dict:
    key_of = jax.random.split(jax.random.key(seed), 4)
    return {
        "queries": draw_queries(jax.random.fold_in(key_of[3], 71), 0),
        "candidates": draw_candidates(jax.random.fold_in(key_of[3], 71), 0),
        "bucket": draw_bucket(jax.random.fold_in(key_of[3], 71), 0),
    }


score_scale = 0.0625
neg_large = -1.0e30


def reference(queries, candidates, bucket):
    ids = bucket[:, 0].astype(jnp.int32)
    order = jnp.argsort(ids, stable=True).astype(jnp.int32)
    span = N_REP * N_DP * CAP
    sorted_q = jnp.concatenate([queries[order].astype(jnp.float32), jnp.zeros((span, E), jnp.float32)], axis=0)
    sorted_c = jnp.concatenate([candidates[order].astype(jnp.float32), jnp.zeros((span, E), jnp.float32)], axis=0)
    order_pad = jnp.concatenate([order, jnp.full((span,), TOKENS, jnp.int32)], axis=0)
    counts = jnp.zeros((N_DP,), jnp.int32).at[ids].add(jnp.ones((TOKENS,), jnp.int32)).astype(jnp.int32)
    starts = (jnp.cumsum(counts) - counts).astype(jnp.int32)

    def one_bucket(item):
        start, count = item
        qrows = lax.dynamic_slice_in_dim(sorted_q, start, span, 0)
        crows = lax.dynamic_slice_in_dim(sorted_c, start, span, 0)
        where_idx = lax.dynamic_slice_in_dim(order_pad, start, span, 0)
        valid = jnp.arange(span, dtype=jnp.int32) < count
        scores = jnp.dot(qrows, crows.T, precision=lax.Precision.HIGHEST) * score_scale
        scores = jnp.where(valid[None, :], scores, neg_large)
        top = jnp.max(scores, axis=1)
        lse = top + jnp.log(jnp.sum(jnp.exp(scores - top[:, None]), axis=1))
        pos = jnp.sum(qrows * crows, axis=1) * score_scale
        count_safe = jnp.maximum(count.astype(jnp.float32), 1.0)
        loss = jnp.where(valid, lse - jnp.log(count_safe) - pos, 0.0)
        idx = jnp.where(valid, where_idx, TOKENS).astype(jnp.int32)
        return loss, idx, jnp.sum(loss) / count_safe

    losses, indices, bucket_loss = lax.map(one_bucket, (starts, counts))
    query_loss = jnp.zeros((TOKENS,), jnp.float32).at[indices.reshape(-1)].set(losses.reshape(-1), mode="drop")
    return query_loss, bucket_loss
```

```python
import math

import jax
import jax.numpy as jnp
from jax import lax
from jax.experimental import pallas as pl
from jax.experimental.pallas import tpu as pltpu
from jax.sharding import PartitionSpec as P

ROWS = 768
WIDTH = 256
HALF = 128
PEERS = 128
CAP = 12
SLOTS = PEERS * CAP
MAIN = PEERS * 8
REST = PEERS * 4
ABSENT = 64.0
NEG = -1e30
LN2 = math.log(2.0)
TO_LOG2 = 0.0625 / LN2

F32 = jnp.float32
BF16 = jnp.bfloat16
VMEM = pl.BlockSpec(memory_space=pltpu.VMEM)


def iota(shape, dim):
    return lax.broadcasted_iota(jnp.int32, shape, dim)


def dot_nn(a, b):
    return lax.dot_general(a, b, (((1,), (0,)), ((), ())), preferred_element_type=F32)


def dot_nt(a, b):
    return lax.dot_general(a, b, (((1,), (1,)), ((), ())), preferred_element_type=F32)


def dot_tn(a, b):
    return lax.dot_general(a, b, (((0,), (0,)), ((), ())), preferred_element_type=F32)


def ranks(b):
    blocks = ROWS // 128
    row = iota((128, 128), 0)
    hot = [(row == b[:, j * 128 : (j + 1) * 128]).astype(F32) for j in range(blocks)]
    stack = jnp.concatenate(hot, axis=0).astype(BF16)
    upper = (iota((128, 256), 0) < iota((128, 256), 1)).astype(F32).astype(BF16)
    both = dot_nn(stack, upper)
    before = jnp.zeros((128, 128), F32)
    rank = []
    for j in range(blocks):
        at = both[j * 128 : (j + 1) * 128]
        rank.append(jnp.sum(hot[j] * (at[:, :128] + before), axis=0, keepdims=True))
        before = before + at[:, 128:]
    return jnp.concatenate(rank, axis=1).astype(jnp.int32), before


def pack_kernel(b_ref, q_ref, c_ref, out_ref):
    b = b_ref[...]
    rank, count = ranks(b)
    main_key = jnp.where(rank < 8, b * 8 + rank, -1)
    rest_key = jnp.where(rank >= 8, b * 8 + rank - 8, -1)
    q = q_ref[...]
    c = c_ref[...]
    step = 32
    for p0 in range(0, PEERS, step):
        n = step * 8
        ids = iota((n, ROWS), 0) + p0 * 8
        main = (ids == main_key).astype(F32).astype(BF16)
        rest = ((ids & ~4) == rest_key).astype(F32).astype(BF16)
        c_main = dot_nn(main, c).reshape(step, 8, WIDTH)
        q_main = dot_nn(main, q).reshape(step, 8, WIDTH)
        c_rest = dot_nn(rest, c).reshape(step, 8, WIDTH)
        q_rest = dot_nn(rest, q).reshape(step, 8, WIDTH)
        slot = iota((step, 8, HALF), 1)
        lane = iota((step, 8, HALF), 2)
        have = jnp.broadcast_to(count[p0 : p0 + step].astype(jnp.int32)[:, None, :], (step, 8, HALF))
        c_lo = jnp.where((lane == 0) & (slot >= have), ABSENT, c_main[:, :, :HALF])
        r_lo = jnp.where(
            slot < 4,
            jnp.where((lane == 0) & (slot + 8 >= have), ABSENT, c_rest[:, :, :HALF]),
            q_rest[:, :, :HALF],
        )
        r_hi = jnp.where(slot < 4, c_rest[:, :, HALF:], q_rest[:, :, HALF:])
        out_ref[p0 : p0 + step, 0:16, :] = jnp.concatenate(
            [c_lo, c_main[:, :, HALF:]], axis=1
        ).astype(BF16)
        out_ref[p0 : p0 + step, 16:32, :] = jnp.concatenate([r_lo, r_hi], axis=1).astype(BF16)
        out_ref[p0 : p0 + step, 32:48, :] = jnp.concatenate(
            [q_main[:, :, :HALF], q_main[:, :, HALF:]], axis=1
        ).astype(BF16)


def unpack_kernel(in_ref, q_ref, c_ref):
    def main_rows(at):
        tile = in_ref[:, at : at + 16, :].astype(F32)
        lo = tile[:, :8, :].reshape(MAIN, HALF)
        hi = tile[:, 8:, :].reshape(MAIN, HALF)
        return lo.astype(BF16), hi.astype(BF16)

    c_lo, c_hi = main_rows(0)
    c_ref[0:MAIN, :HALF] = c_lo
    c_ref[0:MAIN, HALF:] = c_hi
    q_lo, q_hi = main_rows(32)
    q_ref[0:MAIN, :HALF] = q_lo
    q_ref[0:MAIN, HALF:] = q_hi
    tile = in_ref[:, 16:32, :].astype(F32)
    first = iota((PEERS // 2, 8, HALF), 1) < 4
    for half in range(2):
        part = tile[:, half * 8 : half * 8 + 8, :].reshape(PEERS // 2, 2, 8, HALF)
        even = part[:, 0]
        odd = part[:, 1]
        c_part = jnp.where(first, even, pltpu.roll(odd, 4, 1))
        q_part = jnp.where(first, pltpu.roll(even, 4, 1), odd)
        c_ref[MAIN:SLOTS, half * HALF : (half + 1) * HALF] = c_part.reshape(REST, HALF).astype(BF16)
        q_ref[MAIN:SLOTS, half * HALF : (half + 1) * HALF] = q_part.reshape(REST, HALF).astype(BF16)


COLS = 256
CHUNK = 512


def scores_of(q_ref, c_ref, bias_ref, t_ref, done):
    def fill(k, total):
        at = pl.multiple_of(k * CHUNK, CHUNK)
        absent = c_ref[pl.ds(at, CHUNK), 0:1].astype(F32) == ABSENT
        bias_ref[pl.ds(at, CHUNK), :] = jnp.broadcast_to(
            jnp.where(absent, NEG, 0.0), (CHUNK, HALF)
        )
        return total + jnp.sum(jnp.where(absent, 0.0, 1.0), axis=0, keepdims=True)

    count = jnp.zeros((1, 1), F32)
    for k in range(SLOTS // CHUNK):
        count = fill(k, count)

    for j in range(SLOTS // COLS):
        q = q_ref[j * COLS : (j + 1) * COLS, :]
        top = jnp.full((8, COLS), NEG * 2, F32)
        for k in range(SLOTS // CHUNK):
            s = dot_nt(c_ref[k * CHUNK : (k + 1) * CHUNK, :], q)
            bias = bias_ref[k * CHUNK : (k + 1) * CHUNK, :]
            t = s * TO_LOG2 + jnp.concatenate([bias, bias], axis=1)
            t_ref[k * CHUNK : (k + 1) * CHUNK, :] = t
            top = jnp.maximum(top, jnp.max(t.reshape(CHUNK // 8, 8, COLS), axis=0))
        top = jnp.max(top, axis=0, keepdims=True)
        total = jnp.zeros((8, COLS), F32)
        for k in range(SLOTS // CHUNK):
            e = jnp.exp2(t_ref[k * CHUNK : (k + 1) * CHUNK, :] - top)
            total = total + jnp.sum(e.reshape(CHUNK // 8, 8, COLS), axis=0)
        done(j, top, jnp.sum(total, axis=0, keepdims=True))
    return count


def own_kernel(q_ref, c_ref, top_ref, total_ref, count_ref, bias_ref, t_ref):
    def done(j, top, total):
        top_ref[:, j * COLS : (j + 1) * COLS] = top
        total_ref[:, j * COLS : (j + 1) * COLS] = total

    count = scores_of(q_ref, c_ref, bias_ref, t_ref, done)
    count_ref[...] = jnp.broadcast_to(count, (1, 128))


def other_kernel(
    q_ref, own_ref, c_ref, top_ref, total_ref, count_ref, out_ref, sum_ref, n_ref, bias_ref, t_ref, lse_ref
):
    def done(j, top, total):
        top0 = top_ref[:, j * COLS : (j + 1) * COLS]
        total0 = total_ref[:, j * COLS : (j + 1) * COLS]
        new = jnp.maximum(top0, top)
        both = total0 * jnp.exp2(top0 - new) + total * jnp.exp2(top - new)
        lse_ref[:, j * COLS : (j + 1) * COLS] = new * LN2 + jnp.log(both)

    count = scores_of(q_ref, c_ref, bias_ref, t_ref, done) + count_ref[:, 0:1]
    n = jnp.maximum(jnp.broadcast_to(count, (1, 128)), 1.0)
    log_n = jnp.log(n)
    lines = [lse_ref[:, t * 128 : (t + 1) * 128] - log_n for t in range(CAP)]
    lane = iota((1, 128), 1)
    for u in range(PEERS // 8):
        a = lines[u // 2]
        if u % 2:
            a = pltpu.roll(a, 64, 1)
        r = lines[8 + u // 4]
        shift = (64 - 32 * (u % 4)) % 128
        if shift:
            r = pltpu.roll(r, shift, 1)
        line = jnp.where(lane < 64, a, jnp.where(lane < 96, r, 0.0))
        out_ref[u * 8 : (u + 1) * 8, :] = jnp.broadcast_to(line, (8, 128))
    total = lines[0]
    for line in lines[1:]:
        total = total + line
    total = jnp.sum(total, axis=1, keepdims=True)
    total = jnp.where(count > 0, total, 0.0)
    pos = jnp.zeros((8, WIDTH), F32)
    for k in range(SLOTS // CHUNK):
        at = slice(k * CHUNK, (k + 1) * CHUNK)
        both = q_ref[at, :].astype(F32) * own_ref[at, :].astype(F32)
        pos = pos + jnp.sum(both.reshape(CHUNK // 8, 8, WIDTH), axis=0)
    pos = jnp.sum(jnp.sum(pos, axis=0, keepdims=True), axis=1, keepdims=True)
    sum_ref[...] = jnp.broadcast_to(total - pos * 0.0625, (1, 128))
    n_ref[...] = n


def positive_kernel(b_ref, q_ref, c_ref, pos_ref, rank_ref):
    rank, _ = ranks(b_ref[...])
    rank_ref[...] = rank
    both = q_ref[...].astype(F32) * c_ref[...].astype(F32)
    hi = both.astype(BF16)
    lo = (both - hi.astype(F32)).astype(BF16)
    ones = jnp.ones((8, WIDTH), BF16)
    pos_ref[...] = ((dot_nt(ones, hi) + dot_nt(ones, lo)) * 0.0625)[0:1]


def finish_kernel(at_ref, b_ref, rank_ref, pos_ref, back_ref, out_ref):
    me = at_ref[0]
    b = b_ref[...]
    rank = rank_ref[...]
    hot = (iota((PEERS, ROWS), 0) == b).astype(F32).astype(BF16)
    x = back_ref[...]
    hi = x.astype(BF16)
    left = x - hi.astype(F32)
    mid = left.astype(BF16)
    lo = (left - mid.astype(F32)).astype(BF16)
    picked = (dot_tn(hi, hot) + dot_tn(mid, hot)) + dot_tn(lo, hot)
    eighth = me & 7
    lane = jnp.where(rank < 8, eighth * 8 + rank, 64 + eighth * 4 + rank - 8)
    mine = jnp.sum(jnp.where(iota((128, ROWS), 0) == lane, picked, 0.0), axis=0, keepdims=True)
    out_ref[...] = mine - pos_ref[...]


def shards(queries, candidates, bucket):
    b = bucket.reshape(1, ROWS)
    packed = pl.pallas_call(
        pack_kernel,
        out_shape=jax.ShapeDtypeStruct((PEERS, 48, HALF), BF16),
        in_specs=[VMEM] * 3,
        out_specs=VMEM,
        name="pack",
    )(b, queries, candidates)
    received = lax.all_to_all(packed, "dp", split_axis=0, concat_axis=0, tiled=True)
    pos, rank = pl.pallas_call(
        positive_kernel,
        out_shape=(
            jax.ShapeDtypeStruct((1, ROWS), F32),
            jax.ShapeDtypeStruct((1, ROWS), jnp.int32),
        ),
        in_specs=[VMEM] * 3,
        out_specs=(VMEM, VMEM),
        name="positive",
    )(b, queries, candidates)
    slots = jax.ShapeDtypeStruct((SLOTS, WIDTH), BF16)
    own_q, own_c = pl.pallas_call(
        unpack_kernel,
        out_shape=(slots, slots),
        in_specs=[VMEM],
        out_specs=(VMEM, VMEM),
        name="unpack",
    )(received)
    other_c = lax.ppermute(own_c, "rep", [(0, 1), (1, 0)])
    line = jax.ShapeDtypeStruct((1, SLOTS), F32)
    short = jax.ShapeDtypeStruct((1, 128), F32)
    scratch = [pltpu.VMEM((SLOTS, HALF), F32), pltpu.VMEM((SLOTS, COLS), F32)]
    top, total, count = pl.pallas_call(
        own_kernel,
        out_shape=(line, line, short),
        in_specs=[VMEM] * 2,
        out_specs=(VMEM,) * 3,
        scratch_shapes=scratch,
        name="own",
    )(own_q, own_c)
    back, loss_sum, n = pl.pallas_call(
        other_kernel,
        out_shape=(jax.ShapeDtypeStruct((PEERS, 128), F32), short, short),
        in_specs=[VMEM] * 6,
        out_specs=(VMEM,) * 3,
        scratch_shapes=scratch + [pltpu.VMEM((1, SLOTS), F32)],
        name="other",
    )(own_q, own_c, other_c, top, total, count)
    returned = lax.all_to_all(back, "dp", split_axis=0, concat_axis=0, tiled=True)
    loss_total = lax.psum(loss_sum[0, 0], "rep")
    bucket_loss = (loss_total / n[0, 0]).reshape(1)
    me = lax.axis_index("dp").astype(jnp.int32).reshape(1)
    query_loss = pl.pallas_call(
        finish_kernel,
        out_shape=jax.ShapeDtypeStruct((1, ROWS), F32),
        in_specs=[pl.BlockSpec(memory_space=pltpu.SMEM)] + [VMEM] * 4,
        out_specs=VMEM,
        name="finish",
    )(me, b, rank, pos, returned)
    return (query_loss.reshape(ROWS), bucket_loss)


def solution(mesh):
    in_specs = (P(("dp", "rep"), None), P(("dp", "rep"), None), P(("dp", "rep"), None))
    out_specs = (P(("dp", "rep")), P("dp"))
    return jax.shard_map(shards, mesh=mesh, in_specs=in_specs, out_specs=out_specs, check_vma=False)
```

```python
import math

import jax
import jax.numpy as jnp
from jax import lax
from jax.experimental import pallas as pl
from jax.experimental.pallas import tpu as pltpu
from jax.sharding import PartitionSpec as P

ROWS = 768
WIDTH = 256
HALF = 128
PEERS = 128
CAP = 12
SLOTS = PEERS * CAP
MAIN = PEERS * 8
REST = PEERS * 4
ABSENT = 64.0
NEG = -1e30
LN2 = math.log(2.0)
TO_LOG2 = 0.0625 / LN2

F32 = jnp.float32
BF16 = jnp.bfloat16
VMEM = pl.BlockSpec(memory_space=pltpu.VMEM)


def iota(shape, dim):
    return lax.broadcasted_iota(jnp.int32, shape, dim)


def dot_nn(a, b):
    return lax.dot_general(a, b, (((1,), (0,)), ((), ())), preferred_element_type=F32)


def dot_nt(a, b):
    return lax.dot_general(a, b, (((1,), (1,)), ((), ())), preferred_element_type=F32)


def dot_tn(a, b):
    return lax.dot_general(a, b, (((0,), (0,)), ((), ())), preferred_element_type=F32)


def ranks(b):
    blocks = ROWS // 128
    row = iota((128, 128), 0)
    hot = [(row == b[:, j * 128 : (j + 1) * 128]).astype(F32) for j in range(blocks)]
    stack = jnp.concatenate(hot, axis=0).astype(BF16)
    upper = (iota((128, 256), 0) < iota((128, 256), 1)).astype(F32).astype(BF16)
    both = dot_nn(stack, upper)
    before = jnp.zeros((128, 128), F32)
    rank = []
    for j in range(blocks):
        at = both[j * 128 : (j + 1) * 128]
        rank.append(jnp.sum(hot[j] * (at[:, :128] + before), axis=0, keepdims=True))
        before = before + at[:, 128:]
    return jnp.concatenate(rank, axis=1).astype(jnp.int32), before


def pack_kernel(b_ref, q_ref, c_ref, out_ref):
    b = b_ref[...]
    rank, count = ranks(b)
    main_key = jnp.where(rank < 8, b * 8 + rank, -1)
    rest_key = jnp.where(rank >= 8, b * 8 + rank - 8, -1)
    q = q_ref[...]
    c = c_ref[...]
    step = 32
    for p0 in range(0, PEERS, step):
        n = step * 8
        ids = iota((n, ROWS), 0) + p0 * 8
        main = (ids == main_key).astype(F32).astype(BF16)
        rest = ((ids & ~4) == rest_key).astype(F32).astype(BF16)
        c_main = dot_nn(main, c).reshape(step, 8, WIDTH)
        q_main = dot_nn(main, q).reshape(step, 8, WIDTH)
        c_rest = dot_nn(rest, c).reshape(step, 8, WIDTH)
        q_rest = dot_nn(rest, q).reshape(step, 8, WIDTH)
        slot = iota((step, 8, HALF), 1)
        lane = iota((step, 8, HALF), 2)
        have = jnp.broadcast_to(count[p0 : p0 + step].astype(jnp.int32)[:, None, :], (step, 8, HALF))
        c_lo = jnp.where((lane == 0) & (slot >= have), ABSENT, c_main[:, :, :HALF])
        r_lo = jnp.where(
            slot < 4,
            jnp.where((lane == 0) & (slot + 8 >= have), ABSENT, c_rest[:, :, :HALF]),
            q_rest[:, :, :HALF],
        )
        r_hi = jnp.where(slot < 4, c_rest[:, :, HALF:], q_rest[:, :, HALF:])
        out_ref[p0 : p0 + step, 0:16, :] = jnp.concatenate(
            [c_lo, c_main[:, :, HALF:]], axis=1
        ).astype(BF16)
        out_ref[p0 : p0 + step, 16:32, :] = jnp.concatenate([r_lo, r_hi], axis=1).astype(BF16)
        out_ref[p0 : p0 + step, 32:48, :] = jnp.concatenate(
            [q_main[:, :, :HALF], q_main[:, :, HALF:]], axis=1
        ).astype(BF16)


def unpack_kernel(in_ref, q_ref, c_ref, send_ref):
    def main_rows(at):
        tile = in_ref[:, at : at + 16, :].astype(F32)
        lo = tile[:, :8, :].reshape(MAIN, HALF)
        hi = tile[:, 8:, :].reshape(MAIN, HALF)
        return lo.astype(BF16), hi.astype(BF16)

    c_lo, c_hi = main_rows(0)
    c_ref[0:MAIN, :HALF] = c_lo
    c_ref[0:MAIN, HALF:] = c_hi
    q_lo, q_hi = main_rows(32)
    q_ref[0:MAIN, :HALF] = q_lo
    q_ref[0:MAIN, HALF:] = q_hi
    tile = in_ref[:, 16:32, :].astype(F32)
    first = iota((PEERS // 2, 8, HALF), 1) < 4
    for half in range(2):
        part = tile[:, half * 8 : half * 8 + 8, :].reshape(PEERS // 2, 2, 8, HALF)
        even = part[:, 0]
        odd = part[:, 1]
        c_part = jnp.where(first, even, pltpu.roll(odd, 4, 1))
        q_part = jnp.where(first, pltpu.roll(even, 4, 1), odd)
        c_ref[MAIN:SLOTS, half * HALF : (half + 1) * HALF] = c_part.reshape(REST, HALF).astype(BF16)
        q_ref[MAIN:SLOTS, half * HALF : (half + 1) * HALF] = q_part.reshape(REST, HALF).astype(BF16)
    send_ref[...] = c_ref[...]


COLS = 256
CHUNK = 512


def scores_of(q_ref, c_ref, bias_ref, t_ref, done):
    def fill(k, total):
        at = pl.multiple_of(k * CHUNK, CHUNK)
        absent = c_ref[pl.ds(at, CHUNK), 0:1].astype(F32) == ABSENT
        bias_ref[pl.ds(at, CHUNK), :] = jnp.broadcast_to(
            jnp.where(absent, NEG, 0.0), (CHUNK, HALF)
        )
        return total + jnp.sum(jnp.where(absent, 0.0, 1.0), axis=0, keepdims=True)

    count = jnp.zeros((1, 1), F32)
    for k in range(SLOTS // CHUNK):
        count = fill(k, count)

    for j in range(SLOTS // COLS):
        q = q_ref[j * COLS : (j + 1) * COLS, :]
        top = jnp.full((8, COLS), NEG * 2, F32)
        for k in range(SLOTS // CHUNK):
            s = dot_nt(c_ref[k * CHUNK : (k + 1) * CHUNK, :], q)
            bias = bias_ref[k * CHUNK : (k + 1) * CHUNK, :]
            t = s * TO_LOG2 + jnp.concatenate([bias, bias], axis=1)
            t_ref[k * CHUNK : (k + 1) * CHUNK, :] = t
            top = jnp.maximum(top, jnp.max(t.reshape(CHUNK // 8, 8, COLS), axis=0))
        top = jnp.max(top, axis=0, keepdims=True)
        total = jnp.zeros((8, COLS), F32)
        for k in range(SLOTS // CHUNK):
            e = jnp.exp2(t_ref[k * CHUNK : (k + 1) * CHUNK, :] - top)
            total = total + jnp.sum(e.reshape(CHUNK // 8, 8, COLS), axis=0)
        done(j, top, jnp.sum(total, axis=0, keepdims=True))
    return count


def own_kernel(q_ref, c_ref, top_ref, total_ref, count_ref, bias_ref, t_ref):
    def done(j, top, total):
        top_ref[:, j * COLS : (j + 1) * COLS] = top
        total_ref[:, j * COLS : (j + 1) * COLS] = total

    count = scores_of(q_ref, c_ref, bias_ref, t_ref, done)
    count_ref[...] = jnp.broadcast_to(count, (1, 128))


def other_kernel(
    q_ref, own_ref, c_ref, top_ref, total_ref, count_ref, out_ref, sum_ref, n_ref, bias_ref, t_ref, lse_ref
):
    def done(j, top, total):
        top0 = top_ref[:, j * COLS : (j + 1) * COLS]
        total0 = total_ref[:, j * COLS : (j + 1) * COLS]
        new = jnp.maximum(top0, top)
        both = total0 * jnp.exp2(top0 - new) + total * jnp.exp2(top - new)
        lse_ref[:, j * COLS : (j + 1) * COLS] = new * LN2 + jnp.log(both)

    count = scores_of(q_ref, c_ref, bias_ref, t_ref, done) + count_ref[:, 0:1]
    n = jnp.maximum(jnp.broadcast_to(count, (1, 128)), 1.0)
    log_n = jnp.log(n)
    lines = [lse_ref[:, t * 128 : (t + 1) * 128] - log_n for t in range(CAP)]
    lane = iota((1, 128), 1)
    for u in range(PEERS // 8):
        a = lines[u // 2]
        if u % 2:
            a = pltpu.roll(a, 64, 1)
        r = lines[8 + u // 4]
        shift = (64 - 32 * (u % 4)) % 128
        if shift:
            r = pltpu.roll(r, shift, 1)
        line = jnp.where(lane < 64, a, jnp.where(lane < 96, r, 0.0))
        out_ref[u * 8 : (u + 1) * 8, :] = jnp.broadcast_to(line, (8, 128))
    total = lines[0]
    for line in lines[1:]:
        total = total + line
    total = jnp.sum(total, axis=1, keepdims=True)
    total = jnp.where(count > 0, total, 0.0)
    pos = jnp.zeros((8, WIDTH), F32)
    for k in range(SLOTS // CHUNK):
        at = slice(k * CHUNK, (k + 1) * CHUNK)
        both = q_ref[at, :].astype(F32) * own_ref[at, :].astype(F32)
        pos = pos + jnp.sum(both.reshape(CHUNK // 8, 8, WIDTH), axis=0)
    pos = jnp.sum(jnp.sum(pos, axis=0, keepdims=True), axis=1, keepdims=True)
    sum_ref[...] = jnp.broadcast_to(total - pos * 0.0625, (1, 128))
    n_ref[...] = n


def positive_kernel(b_ref, q_ref, c_ref, pos_ref, rank_ref):
    rank, _ = ranks(b_ref[...])
    rank_ref[...] = rank
    both = q_ref[...].astype(F32) * c_ref[...].astype(F32)
    hi = both.astype(BF16)
    lo = (both - hi.astype(F32)).astype(BF16)
    ones = jnp.ones((8, WIDTH), BF16)
    pos_ref[...] = ((dot_nt(ones, hi) + dot_nt(ones, lo)) * 0.0625)[0:1]


def finish_kernel(at_ref, b_ref, rank_ref, pos_ref, back_ref, out_ref):
    me = at_ref[0]
    b = b_ref[...]
    rank = rank_ref[...]
    hot = (iota((PEERS, ROWS), 0) == b).astype(F32).astype(BF16)
    x = back_ref[...]
    hi = x.astype(BF16)
    left = x - hi.astype(F32)
    mid = left.astype(BF16)
    lo = (left - mid.astype(F32)).astype(BF16)
    picked = (dot_tn(hi, hot) + dot_tn(mid, hot)) + dot_tn(lo, hot)
    eighth = me & 7
    lane = jnp.where(rank < 8, eighth * 8 + rank, 64 + eighth * 4 + rank - 8)
    mine = jnp.sum(jnp.where(iota((128, ROWS), 0) == lane, picked, 0.0), axis=0, keepdims=True)
    out_ref[...] = mine - pos_ref[...]


def on_chip(x):
    return pltpu.with_memory_space_constraint(x, pltpu.VMEM)


def shards(queries, candidates, bucket):
    b = bucket.reshape(1, ROWS)
    packed = pl.pallas_call(
        pack_kernel,
        out_shape=pltpu.VMEM((PEERS, 48, HALF), BF16),
        in_specs=[VMEM] * 3,
        out_specs=VMEM,
        name="pack",
    )(b, queries, candidates)
    received = lax.all_to_all(packed, "dp", split_axis=0, concat_axis=0, tiled=True)
    pos, rank = pl.pallas_call(
        positive_kernel,
        out_shape=(
            pltpu.VMEM((1, ROWS), F32),
            pltpu.VMEM((1, ROWS), jnp.int32),
        ),
        in_specs=[VMEM] * 3,
        out_specs=(VMEM, VMEM),
        name="positive",
    )(b, queries, candidates)
    slots = pltpu.VMEM((SLOTS, WIDTH), BF16)
    own_q, own_c, sent_c = pl.pallas_call(
        unpack_kernel,
        out_shape=(slots, slots, jax.ShapeDtypeStruct((SLOTS, WIDTH), BF16)),
        in_specs=[VMEM],
        out_specs=(VMEM,) * 3,
        name="unpack",
    )(on_chip(received))
    other_c = lax.ppermute(sent_c, "rep", [(0, 1), (1, 0)])
    line = pltpu.VMEM((1, SLOTS), F32)
    short = pltpu.VMEM((1, 128), F32)
    scratch = [pltpu.VMEM((SLOTS, HALF), F32), pltpu.VMEM((SLOTS, COLS), F32)]
    top, total, count = pl.pallas_call(
        own_kernel,
        out_shape=(line, line, short),
        in_specs=[VMEM] * 2,
        out_specs=(VMEM,) * 3,
        scratch_shapes=scratch,
        name="own",
    )(on_chip(own_q), on_chip(own_c))
    back, loss_sum, n = pl.pallas_call(
        other_kernel,
        out_shape=(jax.ShapeDtypeStruct((PEERS, 128), F32), short, short),
        in_specs=[VMEM] * 6,
        out_specs=(VMEM,) * 3,
        scratch_shapes=scratch + [pltpu.VMEM((1, SLOTS), F32)],
        name="other",
    )(*[on_chip(x) for x in (own_q, own_c, other_c, top, total, count)])
    returned = lax.all_to_all(back, "dp", split_axis=0, concat_axis=0, tiled=True)
    loss_total = lax.psum(loss_sum[0, 0], "rep")
    bucket_loss = (loss_total / n[0, 0]).reshape(1)
    me = lax.axis_index("dp").astype(jnp.int32).reshape(1)
    query_loss = pl.pallas_call(
        finish_kernel,
        out_shape=jax.ShapeDtypeStruct((1, ROWS), F32),
        in_specs=[pl.BlockSpec(memory_space=pltpu.SMEM)] + [VMEM] * 4,
        out_specs=VMEM,
        name="finish",
    )(me, b, on_chip(rank), on_chip(pos), on_chip(returned))
    return (query_loss.reshape(ROWS), bucket_loss)


def solution(mesh):
    in_specs = (P(("dp", "rep"), None), P(("dp", "rep"), None), P(("dp", "rep"), None))
    out_specs = (P(("dp", "rep")), P("dp"))
    return jax.shard_map(shards, mesh=mesh, in_specs=in_specs, out_specs=out_specs, check_vma=False)
```

```python
import math

import jax
import jax.numpy as jnp
from jax import lax
from jax.experimental import pallas as pl
from jax.experimental.pallas import tpu as pltpu
from jax.sharding import PartitionSpec as P

ROWS = 768
WIDTH = 256
HALF = 128
PEERS = 128
CAP = 12
SLOTS = PEERS * CAP
MAIN = PEERS * 8
REST = PEERS * 4
ABSENT = 64.0
NEG = -1e30
LN2 = math.log(2.0)
TO_LOG2 = 0.0625 / LN2

F32 = jnp.float32
BF16 = jnp.bfloat16
VMEM = pl.BlockSpec(memory_space=pltpu.VMEM)


def iota(shape, dim):
    return lax.broadcasted_iota(jnp.int32, shape, dim)


def dot_nn(a, b):
    return lax.dot_general(a, b, (((1,), (0,)), ((), ())), preferred_element_type=F32)


def dot_nt(a, b):
    return lax.dot_general(a, b, (((1,), (1,)), ((), ())), preferred_element_type=F32)


def dot_tn(a, b):
    return lax.dot_general(a, b, (((0,), (0,)), ((), ())), preferred_element_type=F32)


def ranks(b):
    blocks = ROWS // 128
    row = iota((128, 128), 0)
    hot = [(row == b[:, j * 128 : (j + 1) * 128]).astype(F32) for j in range(blocks)]
    stack = jnp.concatenate(hot, axis=0).astype(BF16)
    upper = (iota((128, 256), 0) < iota((128, 256), 1)).astype(F32).astype(BF16)
    both = dot_nn(stack, upper)
    before = jnp.zeros((128, 128), F32)
    rank = []
    for j in range(blocks):
        at = both[j * 128 : (j + 1) * 128]
        rank.append(jnp.sum(hot[j] * (at[:, :128] + before), axis=0, keepdims=True))
        before = before + at[:, 128:]
    return jnp.concatenate(rank, axis=1).astype(jnp.int32), before


def pack_kernel(b_hbm, q_hbm, c_hbm, out_ref, b_ref, q_ref, c_ref, b_sem, q_sem, c_sem):
    load_b = pltpu.make_async_copy(b_hbm, b_ref, b_sem)
    load_c = pltpu.make_async_copy(c_hbm, c_ref, c_sem)
    load_q = pltpu.make_async_copy(q_hbm, q_ref, q_sem)
    load_b.start()
    load_c.start()
    load_q.start()
    load_b.wait()
    b = b_ref[...]
    rank, count = ranks(b)
    count = count.astype(jnp.int32)
    main_key = jnp.where(rank < 8, b * 8 + rank, -1)
    rest_key = jnp.where(rank >= 8, b * 8 + rank - 8, -1)
    step = 32
    load_c.wait()
    load_q.wait()
    q = q_ref[...]
    c = c_ref[...]
    for p0 in range(0, PEERS, step):
        n = step * 8
        ids = iota((n, ROWS), 0) + p0 * 8
        main = (ids == main_key).astype(F32).astype(BF16)
        rest = ((ids & ~4) == rest_key).astype(F32).astype(BF16)
        c_main = dot_nn(main, c).reshape(step, 8, WIDTH)
        q_main = dot_nn(main, q).reshape(step, 8, WIDTH)
        c_rest = dot_nn(rest, c).reshape(step, 8, WIDTH)
        q_rest = dot_nn(rest, q).reshape(step, 8, WIDTH)
        slot = iota((step, 8, HALF), 1)
        lane = iota((step, 8, HALF), 2)
        have = jnp.broadcast_to(count[p0 : p0 + step][:, None, :], (step, 8, HALF))
        c_lo = jnp.where((lane == 0) & (slot >= have), ABSENT, c_main[:, :, :HALF])
        r_lo = jnp.where(
            slot < 4,
            jnp.where((lane == 0) & (slot + 8 >= have), ABSENT, c_rest[:, :, :HALF]),
            q_rest[:, :, :HALF],
        )
        r_hi = jnp.where(slot < 4, c_rest[:, :, HALF:], q_rest[:, :, HALF:])
        out_ref[p0 : p0 + step, 0:16, :] = jnp.concatenate(
            [c_lo, c_main[:, :, HALF:]], axis=1
        ).astype(BF16)
        out_ref[p0 : p0 + step, 16:32, :] = jnp.concatenate([r_lo, r_hi], axis=1).astype(BF16)
        out_ref[p0 : p0 + step, 32:48, :] = jnp.concatenate(
            [q_main[:, :, :HALF], q_main[:, :, HALF:]], axis=1
        ).astype(BF16)


def main_rows(in_ref, at, ref):
    tile = in_ref[:, at : at + 16, :].astype(F32)
    ref[0:MAIN, :HALF] = tile[:, :8, :].reshape(MAIN, HALF).astype(BF16)
    ref[0:MAIN, HALF:] = tile[:, 8:, :].reshape(MAIN, HALF).astype(BF16)


def rest_rows(in_ref, second, ref):
    tile = in_ref[:, 16:32, :].astype(F32)
    first = iota((PEERS // 2, 8, HALF), 1) < 4
    for half in range(2):
        part = tile[:, half * 8 : half * 8 + 8, :].reshape(PEERS // 2, 2, 8, HALF)
        even = part[:, 0]
        odd = part[:, 1]
        if second:
            rows = jnp.where(first, pltpu.roll(even, 4, 1), odd)
        else:
            rows = jnp.where(first, even, pltpu.roll(odd, 4, 1))
        ref[MAIN:SLOTS, half * HALF : (half + 1) * HALF] = rows.reshape(REST, HALF).astype(BF16)


def candidates_kernel(in_ref, c_ref):
    main_rows(in_ref, 0, c_ref)
    rest_rows(in_ref, False, c_ref)


COLS = 256
CHUNK = 256


def scores_of(q_ref, c_ref, bias_ref, t_ref, done):
    count = jnp.zeros((1, 1), F32)
    for k in range(SLOTS // CHUNK):
        at = slice(k * CHUNK, (k + 1) * CHUNK)
        absent = c_ref[at, 0:1].astype(F32) == ABSENT
        bias_ref[at, :] = jnp.broadcast_to(jnp.where(absent, NEG, 0.0), (CHUNK, HALF))
        count = count + jnp.sum(jnp.where(absent, 0.0, 1.0), axis=0, keepdims=True)

    blocks = SLOTS // COLS
    top = total = None
    for j in range(blocks + 1):
        if j < blocks:
            q = q_ref[j * COLS : (j + 1) * COLS, :]
            new_top = jnp.full((8, COLS), NEG * 2, F32)
        if j > 0:
            total = jnp.zeros((8, COLS), F32)
        for k in range(SLOTS // CHUNK):
            at = slice(k * CHUNK, (k + 1) * CHUNK)
            if j < blocks:
                s = dot_nt(c_ref[at, :], q)
                bias = bias_ref[at, :]
                t = s * TO_LOG2 + jnp.concatenate([bias, bias], axis=1)
                t_ref[j % 2, at, :] = t
                new_top = jnp.maximum(new_top, jnp.max(t.reshape(CHUNK // 8, 8, COLS), axis=0))
            if j > 0:
                e = jnp.exp2(t_ref[(j - 1) % 2, at, :] - top)
                total = total + jnp.sum(e.reshape(CHUNK // 8, 8, COLS), axis=0)
        if j > 0:
            done(j - 1, top, jnp.sum(total, axis=0, keepdims=True))
        if j < blocks:
            top = jnp.max(new_top, axis=0, keepdims=True)
    return count


def own_kernel(in_ref, c_ref, q_ref, top_ref, total_ref, count_ref, bias_ref, t_ref):
    main_rows(in_ref, 32, q_ref)
    rest_rows(in_ref, True, q_ref)

    def done(j, top, total):
        top_ref[:, j * COLS : (j + 1) * COLS] = top
        total_ref[:, j * COLS : (j + 1) * COLS] = total

    count = scores_of(q_ref, c_ref, bias_ref, t_ref, done)
    count_ref[...] = jnp.broadcast_to(count, (1, 128))


def other_kernel(
    q_ref, c_ref, top_ref, total_ref, count_ref, out_ref, lse_ref, n_ref, bias_ref, t_ref
):
    def done(j, top, total):
        top0 = top_ref[:, j * COLS : (j + 1) * COLS]
        total0 = total_ref[:, j * COLS : (j + 1) * COLS]
        new = jnp.maximum(top0, top)
        both = total0 * jnp.exp2(top0 - new) + total * jnp.exp2(top - new)
        lse_ref[:, j * COLS : (j + 1) * COLS] = new * LN2 + jnp.log(both)

    count = scores_of(q_ref, c_ref, bias_ref, t_ref, done) + count_ref[:, 0:1]
    n = jnp.broadcast_to(count, (1, 128))
    n_ref[...] = n
    log_n = jnp.log(jnp.maximum(n, 1.0))
    lines = [lse_ref[:, t * 128 : (t + 1) * 128] - log_n for t in range(CAP)]
    for t in range(CAP):
        lse_ref[:, t * 128 : (t + 1) * 128] = lines[t]
    lane = iota((1, 128), 1)
    for u in range(PEERS // 8):
        a = lines[u // 2]
        if u % 2:
            a = pltpu.roll(a, 64, 1)
        r = lines[8 + u // 4]
        shift = (64 - 32 * (u % 4)) % 128
        if shift:
            r = pltpu.roll(r, shift, 1)
        line = jnp.where(lane < 64, a, jnp.where(lane < 96, r, 0.0))
        out_ref[u * 8 : (u + 1) * 8, :] = jnp.broadcast_to(line, (8, 128))


def sum_kernel(in_ref, lse_ref, n_ref, sum_ref):
    total = jnp.sum(lse_ref[...], axis=1, keepdims=True)
    total = jnp.where(n_ref[:, 0:1] > 0, total, 0.0)
    c = in_ref[:, 0:16, :].astype(F32)
    q = in_ref[:, 32:48, :].astype(F32)
    pos = jnp.sum(c * q, axis=0)
    z = in_ref[:, 16:32, :].astype(F32).reshape(PEERS * 2, 8, HALF)
    low = iota((PEERS * 2, 8, HALF), 1) < 4
    rest = jnp.sum(jnp.where(low, z * pltpu.roll(z, 4, 1), 0.0), axis=0)
    pos = jnp.sum(jnp.sum(pos, axis=0, keepdims=True), axis=1, keepdims=True)
    rest = jnp.sum(jnp.sum(rest, axis=0, keepdims=True), axis=1, keepdims=True)
    sum_ref[...] = jnp.broadcast_to(total - (pos + rest) * 0.0625, (1, 128))


def positive_kernel(at_ref, b_ref, q_ref, c_ref, pos_ref, hot_ref, lane_ref):
    rank, _ = ranks(b_ref[...])
    eighth = at_ref[0] & 7
    lane_ref[...] = jnp.where(rank < 8, eighth * 8 + rank, 64 + eighth * 4 + rank - 8)
    hot_ref[...] = (iota((PEERS, ROWS), 0) == b_ref[...]).astype(F32).astype(BF16)
    both = q_ref[...].astype(F32) * c_ref[...].astype(F32)
    hi = both.astype(BF16)
    lo = (both - hi.astype(F32)).astype(BF16)
    ones = jnp.ones((8, WIDTH), BF16)
    pos_ref[...] = ((dot_nt(ones, hi) + dot_nt(ones, lo)) * 0.0625)[0:1]


def finish_kernel(hot_ref, lane_ref, pos_ref, back_ref, out_ref):
    hot = hot_ref[...]
    x = back_ref[...]
    hi = x.astype(BF16)
    left = x - hi.astype(F32)
    mid = left.astype(BF16)
    lo = (left - mid.astype(F32)).astype(BF16)
    picked = (dot_tn(hi, hot) + dot_tn(mid, hot)) + dot_tn(lo, hot)
    mine = jnp.where(iota((128, ROWS), 0) == lane_ref[...], picked, 0.0)
    mine = jnp.sum(mine, axis=0, keepdims=True) - pos_ref[...]
    for j in range(ROWS // 128):
        out_ref[j : j + 1, :] = mine[:, j * 128 : (j + 1) * 128]


def call(kernel, name, out_shape, *args, specs=None, scratch=()):
    single = not isinstance(out_shape, tuple)
    return pl.pallas_call(
        kernel,
        out_shape=out_shape,
        in_specs=specs or [VMEM] * len(args),
        out_specs=VMEM if single else (VMEM,) * len(out_shape),
        scratch_shapes=scratch,
        compiler_params=pltpu.CompilerParams(vmem_limit_bytes=24 * 1024 * 1024),
        name=name,
    )(*args)


def exchange(x):
    return lax.all_to_all(x, "dp", split_axis=0, concat_axis=0, tiled=True)


def shards(queries, candidates, bucket):
    b = bucket.reshape(1, ROWS)
    me = lax.axis_index("dp").astype(jnp.int32).reshape(1)
    shape = jax.ShapeDtypeStruct
    hbm = pl.BlockSpec(memory_space=pltpu.HBM)
    rows = pltpu.VMEM((ROWS, WIDTH), BF16)
    packed = call(
        pack_kernel, "pack", shape((PEERS, 48, HALF), BF16),
        *[pltpu.with_memory_space_constraint(x, pltpu.HBM) for x in (b, queries, candidates)],
        specs=[hbm] * 3,
        scratch=[pltpu.VMEM((1, ROWS), jnp.int32), rows, rows] + [pltpu.SemaphoreType.DMA] * 3,
    )
    received = exchange(packed)
    own_c = call(candidates_kernel, "candidates", shape((SLOTS, WIDTH), BF16), received)
    other_c = lax.ppermute(own_c, "rep", [(0, 1), (1, 0)])
    line = shape((1, SLOTS), F32)
    short = shape((1, 128), F32)
    scratch = [pltpu.VMEM((SLOTS, HALF), F32), pltpu.VMEM((2, SLOTS, COLS), F32)]
    own_q, top, total, count = call(
        own_kernel, "own", (shape((SLOTS, WIDTH), BF16), line, line, short),
        received, own_c, scratch=scratch,
    )
    back, lse, n = call(
        other_kernel, "other", (shape((PEERS, 128), F32), line, short),
        own_q, other_c, top, total, count, scratch=scratch,
    )
    returned = exchange(back)
    pos, hot, lane = call(
        positive_kernel, "positive",
        (shape((1, ROWS), F32), shape((PEERS, ROWS), BF16), shape((1, ROWS), jnp.int32)),
        me, b, queries, candidates, specs=[pl.BlockSpec(memory_space=pltpu.SMEM)] + [VMEM] * 3,
    )
    loss_sum = call(sum_kernel, "sum", short, received, lse, n)
    loss_total = lax.psum(loss_sum[0, 0], "rep")
    bucket_loss = (loss_total / jnp.maximum(n[0, 0], 1.0)).reshape(1)
    query_loss = call(
        finish_kernel, "finish", shape((ROWS // 128, 128), F32), hot, lane, pos, returned
    )
    return (query_loss.reshape(ROWS), bucket_loss)


def solution(mesh):
    in_specs = (P(("dp", "rep"), None), P(("dp", "rep"), None), P(("dp", "rep"), None))
    out_specs = (P(("dp", "rep")), P("dp"))
    return jax.shard_map(shards, mesh=mesh, in_specs=in_specs, out_specs=out_specs, check_vma=False)
```

```python
import math

import jax
import jax.numpy as jnp
from jax import lax
from jax.experimental import pallas as pl
from jax.experimental.pallas import tpu as pltpu
from jax.sharding import PartitionSpec as P

ROWS = 768
WIDTH = 256
HALF = 128
PEERS = 128
CAP = 12
SLOTS = PEERS * CAP
MAIN = PEERS * 8
REST = PEERS * 4
ABSENT = 64.0
NEG = -1e30
HUGE = 1e37
LN2 = math.log(2.0)
TO_LOG2 = 0.0625 / LN2

F32 = jnp.float32
BF16 = jnp.bfloat16
VMEM = pl.BlockSpec(memory_space=pltpu.VMEM)


def iota(shape, dim):
    return lax.broadcasted_iota(jnp.int32, shape, dim)


def dot_nn(a, b):
    return lax.dot_general(a, b, (((1,), (0,)), ((), ())), preferred_element_type=F32)


def dot_nt(a, b):
    return lax.dot_general(a, b, (((1,), (1,)), ((), ())), preferred_element_type=F32)


def dot_tn(a, b):
    return lax.dot_general(a, b, (((0,), (0,)), ((), ())), preferred_element_type=F32)


def ranks(b):
    blocks = ROWS // 128
    row = iota((128, 128), 0)
    hot = [(row == b[:, j * 128 : (j + 1) * 128]).astype(F32) for j in range(blocks)]
    stack = jnp.concatenate(hot, axis=0).astype(BF16)
    upper = (iota((128, 256), 0) < iota((128, 256), 1)).astype(F32).astype(BF16)
    both = dot_nn(stack, upper)
    before = jnp.zeros((128, 128), F32)
    rank = []
    for j in range(blocks):
        at = both[j * 128 : (j + 1) * 128]
        rank.append(jnp.sum(hot[j] * (at[:, :128] + before), axis=0, keepdims=True))
        before = before + at[:, 128:]
    return jnp.concatenate(rank, axis=1).astype(jnp.int32), before


def pack_kernel(b_hbm, q_hbm, c_hbm, out_ref, b_ref, q_ref, c_ref, b_sem, q_sem, c_sem):
    load_b = pltpu.make_async_copy(b_hbm, b_ref, b_sem)
    load_c = pltpu.make_async_copy(c_hbm, c_ref, c_sem)
    load_q = pltpu.make_async_copy(q_hbm, q_ref, q_sem)
    load_b.start()
    load_c.start()
    load_q.start()
    load_b.wait()
    b = b_ref[...]
    rank, count = ranks(b)
    count = count.astype(jnp.int32)
    main_key = jnp.where(rank < 8, b * 8 + rank, -1)
    rest_key = jnp.where(rank >= 8, b * 4 + rank - 8, -1)
    step = 64
    low = iota((step // 2, 8, WIDTH), 1) < 4
    slot = iota((step, 8, HALF), 1)
    lane = iota((step, 8, HALF), 2)
    load_c.wait()
    load_q.wait()
    q = q_ref[...]
    c = c_ref[...]
    for p0 in range(0, PEERS, step):
        main = (iota((step * 8, ROWS), 0) + p0 * 8 == main_key).astype(F32).astype(BF16)
        rest = (iota((step * 4, ROWS), 0) + p0 * 4 == rest_key).astype(F32).astype(BF16)
        both = jnp.concatenate([main, rest], axis=0)
        c_both = dot_nn(both, c)
        q_both = dot_nn(both, q)
        c_main = c_both[: step * 8].reshape(step, 8, WIDTH)
        q_main = q_both[: step * 8].reshape(step, 8, WIDTH)
        c_rest = c_both[step * 8 :].reshape(step // 2, 8, WIDTH)
        q_rest = q_both[step * 8 :].reshape(step // 2, 8, WIDTH)
        even = jnp.where(low, c_rest, pltpu.roll(q_rest, 4, 1))
        odd = jnp.where(low, pltpu.roll(c_rest, 4, 1), q_rest)
        mixed = jnp.stack([even, odd], axis=1).reshape(step, 8, WIDTH)
        have = jnp.broadcast_to(count[p0 : p0 + step][:, None, :], (step, 8, HALF))
        c_lo = jnp.where((lane == 0) & (slot >= have), ABSENT, c_main[:, :, :HALF])
        gone = (lane == 0) & (slot < 4) & (slot + 8 >= have)
        r_lo = jnp.where(gone, ABSENT, mixed[:, :, :HALF])
        out_ref[p0 : p0 + step, 0:16, :] = jnp.concatenate(
            [c_lo, c_main[:, :, HALF:]], axis=1
        ).astype(BF16)
        out_ref[p0 : p0 + step, 16:32, :] = jnp.concatenate(
            [r_lo, mixed[:, :, HALF:]], axis=1
        ).astype(BF16)
        out_ref[p0 : p0 + step, 32:48, :] = jnp.concatenate(
            [q_main[:, :, :HALF], q_main[:, :, HALF:]], axis=1
        ).astype(BF16)


def main_rows(in_ref, at, ref):
    tile = in_ref[:, at : at + 16, :].astype(F32)
    ref[0:MAIN, :HALF] = tile[:, :8, :].reshape(MAIN, HALF).astype(BF16)
    ref[0:MAIN, HALF:] = tile[:, 8:, :].reshape(MAIN, HALF).astype(BF16)


def rest_rows(in_ref, second, ref):
    tile = in_ref[:, 16:32, :].astype(F32)
    first = iota((PEERS // 2, 8, HALF), 1) < 4
    for half in range(2):
        part = tile[:, half * 8 : half * 8 + 8, :].reshape(PEERS // 2, 2, 8, HALF)
        even = part[:, 0]
        odd = part[:, 1]
        if second:
            rows = jnp.where(first, pltpu.roll(even, 4, 1), odd)
        else:
            rows = jnp.where(first, even, pltpu.roll(odd, 4, 1))
        ref[MAIN:SLOTS, half * HALF : (half + 1) * HALF] = rows.reshape(REST, HALF).astype(BF16)


def candidates_kernel(in_ref, c_ref):
    main_rows(in_ref, 0, c_ref)
    rest_rows(in_ref, False, c_ref)


COLS = 256
CHUNK = 256


def fill_bias(c_ref, bias_ref):
    count = jnp.zeros((1, 1), F32)
    for k in range(SLOTS // CHUNK):
        at = slice(k * CHUNK, (k + 1) * CHUNK)
        absent = c_ref[at, 0:1].astype(F32) == ABSENT
        bias_ref[at, :] = jnp.broadcast_to(jnp.where(absent, NEG, 0.0), (CHUNK, HALF))
        count = count + jnp.sum(jnp.where(absent, 0.0, 1.0), axis=0, keepdims=True)
    return count


def log2_scores(q, c_ref, bias_ref, at):
    bias = bias_ref[at, :]
    return dot_nt(c_ref[at, :], q) * TO_LOG2 + jnp.concatenate([bias, bias], axis=1)


def eights(x, op):
    return op(x.reshape(x.shape[0] // 8, 8, x.shape[1]), axis=0)


def sums(q, c_ref, bias_ref, top, first):
    total = jnp.zeros((8, COLS), F32)
    for at in range(first, SLOTS, CHUNK):
        t = log2_scores(q, c_ref, bias_ref, slice(at, at + CHUNK))
        total = total + eights(jnp.exp2(t - top), jnp.sum)
    return jnp.sum(total, axis=0, keepdims=True)


def exact(q_ref, c_ref, bias_ref, t_ref, done):
    def block(j, _):
        cols = pl.ds(pl.multiple_of(j * COLS, COLS), COLS)
        q = q_ref[cols, :]

        def scores(k, top):
            at = pl.ds(pl.multiple_of(k * CHUNK, CHUNK), CHUNK)
            t = log2_scores(q, c_ref, bias_ref, at)
            t_ref[at, :] = t
            return jnp.maximum(top, eights(t, jnp.max))

        top = lax.fori_loop(0, SLOTS // CHUNK, scores, jnp.full((8, COLS), 2 * NEG, F32))
        top = jnp.max(top, axis=0, keepdims=True)

        def add(k, total):
            at = pl.ds(pl.multiple_of(k * CHUNK, CHUNK), CHUNK)
            return total + eights(jnp.exp2(t_ref[at, :] - top), jnp.sum)

        total = lax.fori_loop(0, SLOTS // CHUNK, add, jnp.zeros((8, COLS), F32))
        done(cols, top, jnp.sum(total, axis=0, keepdims=True))
        return 0

    lax.fori_loop(0, SLOTS // COLS, block, 0)


def too_large(totals):
    worst = totals[0]
    for total in totals[1:]:
        worst = jnp.maximum(worst, total)
    return jnp.max(worst) > HUGE


def own_kernel(in_ref, c_ref, q_ref, top_ref, total_ref, count_ref, bias_ref, t_ref):
    main_rows(in_ref, 32, q_ref)
    rest_rows(in_ref, True, q_ref)
    count_ref[...] = jnp.broadcast_to(fill_bias(c_ref, bias_ref), (1, 128))
    totals = []
    top = None
    for j in range(SLOTS // COLS + 1):
        if j < SLOTS // COLS:
            kept = slice((j % 2) * CHUNK, (j % 2 + 1) * CHUNK)
            t = log2_scores(q_ref[j * COLS : (j + 1) * COLS, :], c_ref, bias_ref, slice(0, CHUNK))
            t_ref[kept, :] = t
            next_top = jnp.max(eights(t, jnp.max), axis=0, keepdims=True)
        if j > 0:
            cols = slice((j - 1) * COLS, j * COLS)
            kept = slice(((j - 1) % 2) * CHUNK, ((j - 1) % 2 + 1) * CHUNK)
            total = jnp.sum(eights(jnp.exp2(t_ref[kept, :] - top), jnp.sum), axis=0, keepdims=True)
            total = total + sums(q_ref[cols, :], c_ref, bias_ref, top, CHUNK)
            top_ref[:, cols] = top
            total_ref[:, cols] = total
            totals.append(total)
        top = next_top

    @pl.when(too_large(totals))
    def _():
        def done(cols, top, total):
            top_ref[:, cols] = top
            total_ref[:, cols] = total

        exact(q_ref, c_ref, bias_ref, t_ref, done)


def other_kernel(
    q_ref, c_ref, top_ref, total_ref, count_ref, out_ref, lse_ref, n_ref, bias_ref, t_ref
):
    count = fill_bias(c_ref, bias_ref) + count_ref[:, 0:1]
    totals = []
    for j in range(SLOTS // COLS):
        cols = slice(j * COLS, (j + 1) * COLS)
        top = top_ref[:, cols]
        total = sums(q_ref[cols, :], c_ref, bias_ref, top, 0)
        lse_ref[:, cols] = top * LN2 + jnp.log(total_ref[:, cols] + total)
        totals.append(total)

    @pl.when(too_large(totals))
    def _():
        def done(cols, top, total):
            top0 = top_ref[:, cols]
            new = jnp.maximum(top0, top)
            both = total_ref[:, cols] * jnp.exp2(top0 - new) + total * jnp.exp2(top - new)
            lse_ref[:, cols] = new * LN2 + jnp.log(both)

        exact(q_ref, c_ref, bias_ref, t_ref, done)

    n = jnp.broadcast_to(count, (1, 128))
    n_ref[...] = n
    log_n = jnp.log(jnp.maximum(n, 1.0))
    lines = [lse_ref[:, t * 128 : (t + 1) * 128] - log_n for t in range(CAP)]
    for t in range(CAP):
        lse_ref[:, t * 128 : (t + 1) * 128] = lines[t]
    lane = iota((1, 128), 1)
    for u in range(PEERS // 8):
        a = lines[u // 2]
        if u % 2:
            a = pltpu.roll(a, 64, 1)
        r = lines[8 + u // 4]
        shift = (64 - 32 * (u % 4)) % 128
        if shift:
            r = pltpu.roll(r, shift, 1)
        line = jnp.where(lane < 64, a, jnp.where(lane < 96, r, 0.0))
        out_ref[u * 8 : (u + 1) * 8, :] = jnp.broadcast_to(line, (8, 128))


def sum_kernel(in_ref, lse_ref, n_ref, sum_ref):
    total = jnp.sum(lse_ref[...], axis=1, keepdims=True)
    total = jnp.where(n_ref[:, 0:1] > 0, total, 0.0)
    c = in_ref[:, 0:16, :].astype(F32)
    q = in_ref[:, 32:48, :].astype(F32)
    pos = jnp.sum(c * q, axis=0)
    z = in_ref[:, 16:32, :].astype(F32).reshape(PEERS * 2, 8, HALF)
    low = iota((PEERS * 2, 8, HALF), 1) < 4
    rest = jnp.sum(jnp.where(low, z * pltpu.roll(z, 4, 1), 0.0), axis=0)
    pos = jnp.sum(jnp.sum(pos, axis=0, keepdims=True), axis=1, keepdims=True)
    rest = jnp.sum(jnp.sum(rest, axis=0, keepdims=True), axis=1, keepdims=True)
    sum_ref[...] = jnp.broadcast_to(total - (pos + rest) * 0.0625, (1, 128))


def positive_kernel(at_ref, b_ref, q_ref, c_ref, pos_ref, hot_ref, lane_ref):
    rank, _ = ranks(b_ref[...])
    eighth = at_ref[0] & 7
    lane_ref[...] = jnp.where(rank < 8, eighth * 8 + rank, 64 + eighth * 4 + rank - 8)
    hot_ref[...] = (iota((PEERS, ROWS), 0) == b_ref[...]).astype(F32).astype(BF16)
    both = q_ref[...].astype(F32) * c_ref[...].astype(F32)
    hi = both.astype(BF16)
    lo = (both - hi.astype(F32)).astype(BF16)
    ones = jnp.ones((8, WIDTH), BF16)
    pos_ref[...] = ((dot_nt(ones, hi) + dot_nt(ones, lo)) * 0.0625)[0:1]


def finish_kernel(hot_ref, lane_ref, pos_ref, back_ref, out_ref):
    hot = hot_ref[...]
    x = back_ref[...]
    hi = x.astype(BF16)
    left = x - hi.astype(F32)
    mid = left.astype(BF16)
    lo = (left - mid.astype(F32)).astype(BF16)
    picked = (dot_tn(hi, hot) + dot_tn(mid, hot)) + dot_tn(lo, hot)
    mine = jnp.where(iota((128, ROWS), 0) == lane_ref[...], picked, 0.0)
    mine = jnp.sum(mine, axis=0, keepdims=True) - pos_ref[...]
    for j in range(ROWS // 128):
        out_ref[j : j + 1, :] = mine[:, j * 128 : (j + 1) * 128]


def call(kernel, name, out_shape, *args, specs=None, scratch=()):
    single = not isinstance(out_shape, tuple)
    return pl.pallas_call(
        kernel,
        out_shape=out_shape,
        in_specs=specs or [VMEM] * len(args),
        out_specs=VMEM if single else (VMEM,) * len(out_shape),
        scratch_shapes=scratch,
        compiler_params=pltpu.CompilerParams(vmem_limit_bytes=24 * 1024 * 1024),
        name=name,
    )(*args)


def exchange(x):
    return lax.all_to_all(x, "dp", split_axis=0, concat_axis=0, tiled=True)


def shards(queries, candidates, bucket):
    b = bucket.reshape(1, ROWS)
    me = lax.axis_index("dp").astype(jnp.int32).reshape(1)
    shape = jax.ShapeDtypeStruct
    hbm = pl.BlockSpec(memory_space=pltpu.HBM)
    rows = pltpu.VMEM((ROWS, WIDTH), BF16)
    packed = call(
        pack_kernel, "pack", shape((PEERS, 48, HALF), BF16),
        *[pltpu.with_memory_space_constraint(x, pltpu.HBM) for x in (b, queries, candidates)],
        specs=[hbm] * 3,
        scratch=[pltpu.VMEM((1, ROWS), jnp.int32), rows, rows] + [pltpu.SemaphoreType.DMA] * 3,
    )
    received = exchange(packed)
    own_c = call(candidates_kernel, "candidates", shape((SLOTS, WIDTH), BF16), received)
    other_c = lax.ppermute(own_c, "rep", [(0, 1), (1, 0)])
    line = shape((1, SLOTS), F32)
    short = shape((1, 128), F32)
    scratch = [pltpu.VMEM((SLOTS, HALF), F32), pltpu.VMEM((SLOTS, COLS), F32)]
    own_q, top, total, count = call(
        own_kernel, "own", (shape((SLOTS, WIDTH), BF16), line, line, short),
        received, own_c, scratch=scratch,
    )
    back, lse, n = call(
        other_kernel, "other", (shape((PEERS, 128), F32), line, short),
        own_q, other_c, top, total, count, scratch=scratch,
    )
    returned = exchange(back)
    pos, hot, lane = call(
        positive_kernel, "positive",
        (shape((1, ROWS), F32), shape((PEERS, ROWS), BF16), shape((1, ROWS), jnp.int32)),
        me, b, queries, candidates, specs=[pl.BlockSpec(memory_space=pltpu.SMEM)] + [VMEM] * 3,
    )
    loss_sum = call(sum_kernel, "sum", short, received, lse, n)
    loss_total = lax.psum(loss_sum[0, 0], "rep")
    bucket_loss = (loss_total / jnp.maximum(n[0, 0], 1.0)).reshape(1)
    query_loss = call(
        finish_kernel, "finish", shape((ROWS // 128, 128), F32), hot, lane, pos, returned
    )
    return (query_loss.reshape(ROWS), bucket_loss)


def solution(mesh):
    in_specs = (P(("dp", "rep"), None), P(("dp", "rep"), None), P(("dp", "rep"), None))
    out_specs = (P(("dp", "rep")), P("dp"))
    return jax.shard_map(shards, mesh=mesh, in_specs=in_specs, out_specs=out_specs, check_vma=False)
```

```python
import math

import jax
import jax.numpy as jnp
from jax import lax
from jax.experimental import pallas as pl
from jax.experimental.pallas import tpu as pltpu
from jax.sharding import PartitionSpec as P

ROWS = 768
WIDTH = 256
HALF = 128
PEERS = 128
CAP = 12
SLOTS = PEERS * CAP
MAIN = PEERS * 8
REST = PEERS * 4
ABSENT = 64.0
NEG = -1e30
HUGE = 1e37
TINY = 1e-25
LN2 = math.log(2.0)
TO_LOG2 = 0.0625 / LN2

F32 = jnp.float32
BF16 = jnp.bfloat16
VMEM = pl.BlockSpec(memory_space=pltpu.VMEM)


def iota(shape, dim):
    return lax.broadcasted_iota(jnp.int32, shape, dim)


def dot_nn(a, b):
    return lax.dot_general(a, b, (((1,), (0,)), ((), ())), preferred_element_type=F32)


def dot_nt(a, b):
    return lax.dot_general(a, b, (((1,), (1,)), ((), ())), preferred_element_type=F32)


def dot_tn(a, b):
    return lax.dot_general(a, b, (((0,), (0,)), ((), ())), preferred_element_type=F32)


def ranks(b):
    blocks = ROWS // 128
    row = iota((128, 128), 0)
    hot = [(row == b[:, j * 128 : (j + 1) * 128]).astype(F32) for j in range(blocks)]
    stack = jnp.concatenate(hot, axis=0).astype(BF16)
    upper = (iota((128, 256), 0) < iota((128, 256), 1)).astype(F32).astype(BF16)
    both = dot_nn(stack, upper)
    before = jnp.zeros((128, 128), F32)
    rank = []
    for j in range(blocks):
        at = both[j * 128 : (j + 1) * 128]
        rank.append(jnp.sum(hot[j] * (at[:, :128] + before), axis=0, keepdims=True))
        before = before + at[:, 128:]
    return jnp.concatenate(rank, axis=1).astype(jnp.int32), before


def pack_kernel(b_hbm, q_hbm, c_hbm, out_ref, b_ref, q_ref, c_ref, b_sem, q_sem, c_sem):
    load_b = pltpu.make_async_copy(b_hbm, b_ref, b_sem)
    load_c = pltpu.make_async_copy(c_hbm, c_ref, c_sem)
    load_q = pltpu.make_async_copy(q_hbm, q_ref, q_sem)
    load_b.start()
    load_c.start()
    load_q.start()
    load_b.wait()
    b = b_ref[...]
    rank, count = ranks(b)
    count = count.astype(jnp.int32)
    main_key = jnp.where(rank < 8, b * 8 + rank, -1)
    rest_key = jnp.where(rank >= 8, b * 4 + rank - 8, -1)
    step = 64
    low = iota((step // 2, 8, WIDTH), 1) < 4
    slot = iota((step, 8, HALF), 1)
    lane = iota((step, 8, HALF), 2)
    load_c.wait()
    load_q.wait()
    q = q_ref[...]
    c = c_ref[...]
    for p0 in range(0, PEERS, step):
        main = (iota((step * 8, ROWS), 0) + p0 * 8 == main_key).astype(F32).astype(BF16)
        rest = (iota((step * 4, ROWS), 0) + p0 * 4 == rest_key).astype(F32).astype(BF16)
        both = jnp.concatenate([main, rest], axis=0)
        c_both = dot_nn(both, c)
        q_both = dot_nn(both, q)
        c_main = c_both[: step * 8].reshape(step, 8, WIDTH)
        q_main = q_both[: step * 8].reshape(step, 8, WIDTH)
        c_rest = c_both[step * 8 :].reshape(step // 2, 8, WIDTH)
        q_rest = q_both[step * 8 :].reshape(step // 2, 8, WIDTH)
        even = jnp.where(low, c_rest, pltpu.roll(q_rest, 4, 1))
        odd = jnp.where(low, pltpu.roll(c_rest, 4, 1), q_rest)
        mixed = jnp.stack([even, odd], axis=1).reshape(step, 8, WIDTH)
        have = jnp.broadcast_to(count[p0 : p0 + step][:, None, :], (step, 8, HALF))
        c_lo = jnp.where((lane == 0) & (slot >= have), ABSENT, c_main[:, :, :HALF])
        gone = (lane == 0) & (slot < 4) & (slot + 8 >= have)
        r_lo = jnp.where(gone, ABSENT, mixed[:, :, :HALF])
        out_ref[p0 : p0 + step, 0:16, :] = jnp.concatenate(
            [c_lo, c_main[:, :, HALF:]], axis=1
        ).astype(BF16)
        out_ref[p0 : p0 + step, 16:32, :] = jnp.concatenate(
            [r_lo, mixed[:, :, HALF:]], axis=1
        ).astype(BF16)
        out_ref[p0 : p0 + step, 32:48, :] = jnp.concatenate(
            [q_main[:, :, :HALF], q_main[:, :, HALF:]], axis=1
        ).astype(BF16)


def main_rows(in_ref, at, ref):
    tile = in_ref[:, at : at + 16, :].astype(F32)
    ref[0:MAIN, :HALF] = tile[:, :8, :].reshape(MAIN, HALF).astype(BF16)
    ref[0:MAIN, HALF:] = tile[:, 8:, :].reshape(MAIN, HALF).astype(BF16)


def rest_rows(in_ref, second, ref):
    tile = in_ref[:, 16:32, :].astype(F32)
    first = iota((PEERS // 2, 8, HALF), 1) < 4
    for half in range(2):
        part = tile[:, half * 8 : half * 8 + 8, :].reshape(PEERS // 2, 2, 8, HALF)
        even = part[:, 0]
        odd = part[:, 1]
        if second:
            rows = jnp.where(first, pltpu.roll(even, 4, 1), odd)
        else:
            rows = jnp.where(first, even, pltpu.roll(odd, 4, 1))
        ref[MAIN:SLOTS, half * HALF : (half + 1) * HALF] = rows.reshape(REST, HALF).astype(BF16)


def candidates_kernel(in_ref, c_ref):
    main_rows(in_ref, 0, c_ref)
    rest_rows(in_ref, False, c_ref)


COLS = 256
CHUNK = 256


def eights(x, op):
    return op(x.reshape(x.shape[0] // 8, 8, x.shape[1]), axis=0)


def zeroed(c_ref, lo_ref):
    gone = jnp.zeros((8, HALF), F32)
    for k in range(SLOTS // CHUNK):
        at = slice(k * CHUNK, (k + 1) * CHUNK)
        x = c_ref[at, :HALF].astype(F32)
        absent = x == ABSENT
        lo_ref[at, :] = jnp.where(absent, 0.0, x).astype(BF16)
        gone = gone + eights(jnp.where(absent, 1.0, 0.0), jnp.sum)
    return jnp.sum(jnp.sum(gone, axis=0, keepdims=True), axis=1, keepdims=True)


def sums(q, c_ref, lo_ref):
    total = jnp.zeros((8, COLS), F32)
    for k in range(SLOTS // CHUNK):
        at = slice(k * CHUNK, (k + 1) * CHUNK)
        rows = jnp.concatenate([lo_ref[at, :], c_ref[at, HALF:]], axis=1)
        total = total + eights(jnp.exp2(dot_nt(rows, q) * TO_LOG2), jnp.sum)
    return jnp.sum(total, axis=0, keepdims=True)


def exact(q_ref, c_refs, t_ref, lse_ref):
    steps = SLOTS // CHUNK

    def block(j, _):
        cols = pl.ds(pl.multiple_of(j * COLS, COLS), COLS)
        q = q_ref[cols, :]
        top = jnp.full((8, COLS), 2 * NEG, F32)
        for i, c_ref in enumerate(c_refs):

            def scores(k, top):
                at = pl.ds(pl.multiple_of(k * CHUNK, CHUNK), CHUNK)
                rows = c_ref[at, :]
                absent = rows[:, 0:1].astype(F32) == ABSENT
                t = dot_nt(rows, q) * TO_LOG2 + jnp.where(absent, NEG, 0.0)
                t_ref[i, at, :] = t
                return jnp.maximum(top, eights(t, jnp.max))

            top = lax.fori_loop(0, steps, scores, top)
        top = jnp.max(top, axis=0, keepdims=True)
        total = jnp.zeros((8, COLS), F32)
        for i in range(len(c_refs)):

            def add(k, total):
                at = pl.ds(pl.multiple_of(k * CHUNK, CHUNK), CHUNK)
                return total + eights(jnp.exp2(t_ref[i, at, :] - top), jnp.sum)

            total = lax.fori_loop(0, steps, add, total)
        lse_ref[:, cols] = top * LN2 + jnp.log(jnp.sum(total, axis=0, keepdims=True))
        return 0

    lax.fori_loop(0, SLOTS // COLS, block, 0)


def own_kernel(in_ref, c_ref, q_ref, total_ref, gone_ref, lo_ref):
    main_rows(in_ref, 32, q_ref)
    rest_rows(in_ref, True, q_ref)
    gone_ref[...] = jnp.broadcast_to(zeroed(c_ref, lo_ref), (1, 128))
    for j in range(SLOTS // COLS):
        cols = slice(j * COLS, (j + 1) * COLS)
        total_ref[:, cols] = sums(q_ref[cols, :], c_ref, lo_ref)


def other_kernel(
    q_ref, own_ref, c_ref, total_ref, gone_ref, out_ref, lse_ref, n_ref, lo_ref, t_ref
):
    gone = zeroed(c_ref, lo_ref) + gone_ref[:, 0:1]
    count = 2 * SLOTS - gone
    most = least = None
    for j in range(SLOTS // COLS):
        cols = slice(j * COLS, (j + 1) * COLS)
        total = total_ref[:, cols] + sums(q_ref[cols, :], c_ref, lo_ref)
        present = total - gone
        lse_ref[:, cols] = jnp.log(jnp.maximum(present, TINY))
        most = total if j == 0 else jnp.maximum(most, total)
        least = present if j == 0 else jnp.minimum(least, present)
    most = jnp.max(most, axis=1, keepdims=True)
    least = jnp.min(least, axis=1, keepdims=True)
    redo = (count > 0) & ((most > HUGE) | (least < 0.25 * gone + TINY))

    @pl.when(jnp.max(jnp.where(redo, 1.0, 0.0)) > 0)
    def _():
        exact(q_ref, (own_ref, c_ref), t_ref, lse_ref)

    n = jnp.broadcast_to(count, (1, 128))
    n_ref[...] = n
    log_n = jnp.log(jnp.maximum(n, 1.0))
    lines = [lse_ref[:, t * 128 : (t + 1) * 128] - log_n for t in range(CAP)]
    for t in range(CAP):
        lse_ref[:, t * 128 : (t + 1) * 128] = lines[t]
    lane = iota((1, 128), 1)
    for u in range(PEERS // 8):
        a = lines[u // 2]
        if u % 2:
            a = pltpu.roll(a, 64, 1)
        r = lines[8 + u // 4]
        shift = (64 - 32 * (u % 4)) % 128
        if shift:
            r = pltpu.roll(r, shift, 1)
        line = jnp.where(lane < 64, a, jnp.where(lane < 96, r, 0.0))
        out_ref[u * 8 : (u + 1) * 8, :] = jnp.broadcast_to(line, (8, 128))


def sum_kernel(in_ref, lse_ref, n_ref, sum_ref):
    total = jnp.sum(lse_ref[...], axis=1, keepdims=True)
    total = jnp.where(n_ref[:, 0:1] > 0, total, 0.0)
    c = in_ref[:, 0:16, :].astype(F32)
    q = in_ref[:, 32:48, :].astype(F32)
    pos = jnp.sum(c * q, axis=0)
    z = in_ref[:, 16:32, :].astype(F32).reshape(PEERS * 2, 8, HALF)
    low = iota((PEERS * 2, 8, HALF), 1) < 4
    rest = jnp.sum(jnp.where(low, z * pltpu.roll(z, 4, 1), 0.0), axis=0)
    pos = jnp.sum(jnp.sum(pos, axis=0, keepdims=True), axis=1, keepdims=True)
    rest = jnp.sum(jnp.sum(rest, axis=0, keepdims=True), axis=1, keepdims=True)
    sum_ref[...] = jnp.broadcast_to(total - (pos + rest) * 0.0625, (1, 128))


def positive_kernel(at_ref, b_ref, q_ref, c_ref, pos_ref, hot_ref, lane_ref):
    rank, _ = ranks(b_ref[...])
    eighth = at_ref[0] & 7
    lane_ref[...] = jnp.where(rank < 8, eighth * 8 + rank, 64 + eighth * 4 + rank - 8)
    hot_ref[...] = (iota((PEERS, ROWS), 0) == b_ref[...]).astype(F32).astype(BF16)
    both = q_ref[...].astype(F32) * c_ref[...].astype(F32)
    hi = both.astype(BF16)
    lo = (both - hi.astype(F32)).astype(BF16)
    ones = jnp.ones((8, WIDTH), BF16)
    pos_ref[...] = ((dot_nt(ones, hi) + dot_nt(ones, lo)) * 0.0625)[0:1]


def finish_kernel(hot_ref, lane_ref, pos_ref, back_ref, out_ref):
    hot = hot_ref[...]
    x = back_ref[...]
    hi = x.astype(BF16)
    left = x - hi.astype(F32)
    mid = left.astype(BF16)
    lo = (left - mid.astype(F32)).astype(BF16)
    picked = (dot_tn(hi, hot) + dot_tn(mid, hot)) + dot_tn(lo, hot)
    mine = jnp.where(iota((128, ROWS), 0) == lane_ref[...], picked, 0.0)
    mine = jnp.sum(mine, axis=0, keepdims=True) - pos_ref[...]
    for j in range(ROWS // 128):
        out_ref[j : j + 1, :] = mine[:, j * 128 : (j + 1) * 128]


def call(kernel, name, out_shape, *args, specs=None, scratch=()):
    single = not isinstance(out_shape, tuple)
    return pl.pallas_call(
        kernel,
        out_shape=out_shape,
        in_specs=specs or [VMEM] * len(args),
        out_specs=VMEM if single else (VMEM,) * len(out_shape),
        scratch_shapes=scratch,
        compiler_params=pltpu.CompilerParams(vmem_limit_bytes=24 * 1024 * 1024),
        name=name,
    )(*args)


def exchange(x):
    return lax.all_to_all(x, "dp", split_axis=0, concat_axis=0, tiled=True)


def shards(queries, candidates, bucket):
    b = bucket.reshape(1, ROWS)
    me = lax.axis_index("dp").astype(jnp.int32).reshape(1)
    shape = jax.ShapeDtypeStruct
    hbm = pl.BlockSpec(memory_space=pltpu.HBM)
    rows = pltpu.VMEM((ROWS, WIDTH), BF16)
    packed = call(
        pack_kernel, "pack", shape((PEERS, 48, HALF), BF16),
        *[pltpu.with_memory_space_constraint(x, pltpu.HBM) for x in (b, queries, candidates)],
        specs=[hbm] * 3,
        scratch=[pltpu.VMEM((1, ROWS), jnp.int32), rows, rows] + [pltpu.SemaphoreType.DMA] * 3,
    )
    received = exchange(packed)
    own_c = call(candidates_kernel, "candidates", shape((SLOTS, WIDTH), BF16), received)
    other_c = lax.ppermute(own_c, "rep", [(0, 1), (1, 0)])
    line = shape((1, SLOTS), F32)
    short = shape((1, 128), F32)
    low = pltpu.VMEM((SLOTS, HALF), BF16)
    own_q, total, gone = call(
        own_kernel, "own", (shape((SLOTS, WIDTH), BF16), line, short),
        received, own_c, scratch=[low],
    )
    back, lse, n = call(
        other_kernel, "other", (shape((PEERS, 128), F32), line, short),
        own_q, own_c, other_c, total, gone,
        scratch=[low, pltpu.VMEM((2, SLOTS, COLS), F32)],
    )
    returned = exchange(back)
    pos, hot, lane = call(
        positive_kernel, "positive",
        (shape((1, ROWS), F32), shape((PEERS, ROWS), BF16), shape((1, ROWS), jnp.int32)),
        me, b, queries, candidates, specs=[pl.BlockSpec(memory_space=pltpu.SMEM)] + [VMEM] * 3,
    )
    loss_sum = call(sum_kernel, "sum", short, received, lse, n)
    loss_total = lax.psum(loss_sum[0, 0], "rep")
    bucket_loss = (loss_total / jnp.maximum(n[0, 0], 1.0)).reshape(1)
    query_loss = call(
        finish_kernel, "finish", shape((ROWS // 128, 128), F32), hot, lane, pos, returned
    )
    return (query_loss.reshape(ROWS), bucket_loss)


def solution(mesh):
    in_specs = (P(("dp", "rep"), None), P(("dp", "rep"), None), P(("dp", "rep"), None))
    out_specs = (P(("dp", "rep")), P("dp"))
    return jax.shard_map(shards, mesh=mesh, in_specs=in_specs, out_specs=out_specs, check_vma=False)
```

```python
import math

import jax
import jax.numpy as jnp
from jax import lax
from jax.experimental import pallas as pl
from jax.experimental.pallas import tpu as pltpu
from jax.sharding import PartitionSpec as P


ROWS = 768
WIDTH = 256
HALF = 128
PEERS = 128
CAP = 12
SLOTS = PEERS * CAP
MAIN = PEERS * 8
REST = PEERS * 4
ABSENT = 64.0
NEG = -1e30
HUGE = 1e37
TINY = 1e-25
LN2 = math.log(2.0)
TO_LOG2 = 0.0625 / LN2

F32 = jnp.float32
BF16 = jnp.bfloat16
VMEM = pl.BlockSpec(memory_space=pltpu.VMEM)


def iota(shape, dim):
    return lax.broadcasted_iota(jnp.int32, shape, dim)


def dot_nn(a, b):
    return lax.dot_general(a, b, (((1,), (0,)), ((), ())), preferred_element_type=F32)


def dot_nt(a, b):
    return lax.dot_general(a, b, (((1,), (1,)), ((), ())), preferred_element_type=F32)


def dot_tn(a, b):
    return lax.dot_general(a, b, (((0,), (0,)), ((), ())), preferred_element_type=F32)


def ranks(b):
    blocks = ROWS // 128
    row = iota((128, 128), 0)
    hot = [(row == b[:, j * 128 : (j + 1) * 128]).astype(F32) for j in range(blocks)]
    stack = jnp.concatenate(hot, axis=0).astype(BF16)
    upper = (iota((128, 256), 0) < iota((128, 256), 1)).astype(F32).astype(BF16)
    both = dot_nn(stack, upper)
    before = jnp.zeros((128, 128), F32)
    rank = []
    for j in range(blocks):
        at = both[j * 128 : (j + 1) * 128]
        rank.append(jnp.sum(hot[j] * (at[:, :128] + before), axis=0, keepdims=True))
        before = before + at[:, 128:]
    return jnp.concatenate(rank, axis=1).astype(jnp.int32), before


def pack_kernel(
    b_hbm, q_hbm, c_hbm, out_ref, rank_ref, pos_ref, b_ref, q_ref, c_ref, b_sem, q_sem, c_sem
):
    load_b = pltpu.make_async_copy(b_hbm, b_ref, b_sem)
    load_c = pltpu.make_async_copy(c_hbm, c_ref, c_sem)
    load_q = pltpu.make_async_copy(q_hbm, q_ref, q_sem)
    load_b.start()
    load_c.start()
    load_q.start()
    load_b.wait()
    b = b_ref[...]
    rank, count = ranks(b)
    rank_ref[...] = rank
    count = count.astype(jnp.int32)
    main_key = jnp.where(rank < 8, b * 8 + rank, -1)
    rest_key = jnp.where(rank >= 8, b * 4 + rank - 8, -1)
    step = 64
    low = iota((step // 2, 8, WIDTH), 1) < 4
    slot = iota((step, 8, HALF), 1)
    lane = iota((step, 8, HALF), 2)
    load_c.wait()
    load_q.wait()
    q = q_ref[...]
    c = c_ref[...]
    for p0 in range(0, PEERS, step):
        main = (iota((step * 8, ROWS), 0) + p0 * 8 == main_key).astype(F32).astype(BF16)
        rest = (iota((step * 4, ROWS), 0) + p0 * 4 == rest_key).astype(F32).astype(BF16)
        both = jnp.concatenate([main, rest], axis=0)
        c_both = dot_nn(both, c)
        q_both = dot_nn(both, q)
        c_main = c_both[: step * 8].reshape(step, 8, WIDTH)
        q_main = q_both[: step * 8].reshape(step, 8, WIDTH)
        c_rest = c_both[step * 8 :].reshape(step // 2, 8, WIDTH)
        q_rest = q_both[step * 8 :].reshape(step // 2, 8, WIDTH)
        even = jnp.where(low, c_rest, pltpu.roll(q_rest, 4, 1))
        odd = jnp.where(low, pltpu.roll(c_rest, 4, 1), q_rest)
        mixed = jnp.stack([even, odd], axis=1).reshape(step, 8, WIDTH)
        have = jnp.broadcast_to(count[p0 : p0 + step][:, None, :], (step, 8, HALF))
        c_lo = jnp.where((lane == 0) & (slot >= have), ABSENT, c_main[:, :, :HALF])
        gone = (lane == 0) & (slot < 4) & (slot + 8 >= have)
        r_lo = jnp.where(gone, ABSENT, mixed[:, :, :HALF])
        out_ref[p0 : p0 + step, 0:16, :] = jnp.concatenate(
            [c_lo, c_main[:, :, HALF:]], axis=1
        ).astype(BF16)
        out_ref[p0 : p0 + step, 16:32, :] = jnp.concatenate(
            [r_lo, mixed[:, :, HALF:]], axis=1
        ).astype(BF16)
        out_ref[p0 : p0 + step, 32:48, :] = jnp.concatenate(
            [q_main[:, :, :HALF], q_main[:, :, HALF:]], axis=1
        ).astype(BF16)
    both = q.astype(F32) * c.astype(F32)
    hi = both.astype(BF16)
    lo = (both - hi.astype(F32)).astype(BF16)
    ones = jnp.ones((8, WIDTH), BF16)
    pos_ref[...] = ((dot_nt(ones, hi) + dot_nt(ones, lo)) * 0.0625)[0:1]


def main_rows(in_ref, at, ref):
    tile = in_ref[:, at : at + 16, :].astype(F32)
    ref[0:MAIN, :HALF] = tile[:, :8, :].reshape(MAIN, HALF).astype(BF16)
    ref[0:MAIN, HALF:] = tile[:, 8:, :].reshape(MAIN, HALF).astype(BF16)


def rest_rows(in_ref, second, ref):
    tile = in_ref[:, 16:32, :].astype(F32)
    first = iota((PEERS // 2, 8, HALF), 1) < 4
    for half in range(2):
        part = tile[:, half * 8 : half * 8 + 8, :].reshape(PEERS // 2, 2, 8, HALF)
        even = part[:, 0]
        odd = part[:, 1]
        if second:
            rows = jnp.where(first, pltpu.roll(even, 4, 1), odd)
        else:
            rows = jnp.where(first, even, pltpu.roll(odd, 4, 1))
        ref[MAIN:SLOTS, half * HALF : (half + 1) * HALF] = rows.reshape(REST, HALF).astype(BF16)


def candidates_kernel(in_ref, c_ref):
    main_rows(in_ref, 0, c_ref)
    rest_rows(in_ref, False, c_ref)


COLS = 256
CHUNK = 256


def eights(x, op):
    return op(x.reshape(x.shape[0] // 8, 8, x.shape[1]), axis=0)


def zeroed(c_ref, lo_ref):
    gone = jnp.zeros((8, HALF), F32)
    for k in range(SLOTS // CHUNK):
        at = slice(k * CHUNK, (k + 1) * CHUNK)
        x = c_ref[at, :HALF].astype(F32)
        absent = x == ABSENT
        lo_ref[at, :] = jnp.where(absent, 0.0, x).astype(BF16)
        gone = gone + eights(jnp.where(absent, 1.0, 0.0), jnp.sum)
    return jnp.sum(jnp.sum(gone, axis=0, keepdims=True), axis=1, keepdims=True)


def sums(q, c_ref, lo_ref):
    total = jnp.zeros((8, COLS), F32)
    for k in range(SLOTS // CHUNK):
        at = slice(k * CHUNK, (k + 1) * CHUNK)
        rows = jnp.concatenate([lo_ref[at, :], c_ref[at, HALF:]], axis=1)
        total = total + eights(jnp.exp2(dot_nt(rows, q) * TO_LOG2), jnp.sum)
    return jnp.sum(total, axis=0, keepdims=True)


def exact(q_ref, c_refs, t_ref, lse_ref):
    steps = SLOTS // CHUNK

    def block(j, _):
        cols = pl.ds(pl.multiple_of(j * COLS, COLS), COLS)
        q = q_ref[cols, :]
        top = jnp.full((8, COLS), 2 * NEG, F32)
        for i, c_ref in enumerate(c_refs):

            def scores(k, top):
                at = pl.ds(pl.multiple_of(k * CHUNK, CHUNK), CHUNK)
                rows = c_ref[at, :]
                absent = rows[:, 0:1].astype(F32) == ABSENT
                t = dot_nt(rows, q) * TO_LOG2 + jnp.where(absent, NEG, 0.0)
                t_ref[i, at, :] = t
                return jnp.maximum(top, eights(t, jnp.max))

            top = lax.fori_loop(0, steps, scores, top)
        top = jnp.max(top, axis=0, keepdims=True)
        total = jnp.zeros((8, COLS), F32)
        for i in range(len(c_refs)):

            def add(k, total):
                at = pl.ds(pl.multiple_of(k * CHUNK, CHUNK), CHUNK)
                return total + eights(jnp.exp2(t_ref[i, at, :] - top), jnp.sum)

            total = lax.fori_loop(0, steps, add, total)
        lse_ref[:, cols] = top * LN2 + jnp.log(jnp.sum(total, axis=0, keepdims=True))
        return 0

    lax.fori_loop(0, SLOTS // COLS, block, 0)


def own_kernel(in_ref, c_ref, q_ref, total_ref, gone_ref, pos_ref, lo_ref):
    main_rows(in_ref, 32, q_ref)
    rest_rows(in_ref, True, q_ref)
    gone_ref[...] = jnp.broadcast_to(zeroed(c_ref, lo_ref), (1, 128))
    for j in range(SLOTS // COLS):
        cols = slice(j * COLS, (j + 1) * COLS)
        total_ref[:, cols] = sums(q_ref[cols, :], c_ref, lo_ref)
    pos = jnp.zeros((8, WIDTH), F32)
    for k in range(SLOTS // CHUNK):
        at = slice(k * CHUNK, (k + 1) * CHUNK)
        pos = pos + eights(q_ref[at, :].astype(F32) * c_ref[at, :].astype(F32), jnp.sum)
    pos_ref[...] = jnp.sum(pos, axis=0, keepdims=True)[:, :HALF] + jnp.sum(pos, axis=0, keepdims=True)[:, HALF:]


def other_kernel(
    q_ref, own_ref, c_ref, total_ref, gone_ref, pos_ref, out_ref, sum_ref, n_ref, lo_ref, t_ref, lse_ref
):
    gone = zeroed(c_ref, lo_ref) + gone_ref[:, 0:1]
    count = 2 * SLOTS - gone
    most = least = None
    for j in range(SLOTS // COLS):
        cols = slice(j * COLS, (j + 1) * COLS)
        total = total_ref[:, cols] + sums(q_ref[cols, :], c_ref, lo_ref)
        present = total - gone
        lse_ref[:, cols] = jnp.log(jnp.maximum(present, TINY))
        most = total if j == 0 else jnp.maximum(most, total)
        least = present if j == 0 else jnp.minimum(least, present)
    most = jnp.max(most, axis=1, keepdims=True)
    least = jnp.min(least, axis=1, keepdims=True)
    redo = (count > 0) & ((most > HUGE) | (least < 0.25 * gone + TINY))

    @pl.when(jnp.max(jnp.where(redo, 1.0, 0.0)) > 0)
    def _():
        exact(q_ref, (own_ref, c_ref), t_ref, lse_ref)

    n = jnp.broadcast_to(count, (1, 128))
    n_ref[...] = n
    log_n = jnp.log(jnp.maximum(n, 1.0))
    lines = [lse_ref[:, t * 128 : (t + 1) * 128] - log_n for t in range(CAP)]
    loss = lines[0]
    for line in lines[1:]:
        loss = loss + line
    loss = jnp.sum(loss - pos_ref[...] * 0.0625, axis=1, keepdims=True)
    sum_ref[...] = jnp.broadcast_to(jnp.where(count > 0, loss, 0.0), (1, 128))
    lane = iota((1, 128), 1)
    for u in range(PEERS // 8):
        a = lines[u // 2]
        if u % 2:
            a = pltpu.roll(a, 64, 1)
        r = lines[8 + u // 4]
        shift = (64 - 32 * (u % 4)) % 128
        if shift:
            r = pltpu.roll(r, shift, 1)
        line = jnp.where(lane < 64, a, jnp.where(lane < 96, r, 0.0))
        out_ref[u * 8 : (u + 1) * 8, :] = jnp.broadcast_to(line, (8, 128))


def finish_kernel(b_ref, rank_ref, pos_ref, back_ref, out_ref):
    eighth = lax.axis_index("dp") & 7
    rank = rank_ref[...]
    lane = jnp.where(rank < 8, eighth * 8 + rank, 64 + eighth * 4 + rank - 8)
    hot = (iota((PEERS, ROWS), 0) == b_ref[...]).astype(F32).astype(BF16)
    x = back_ref[...]
    hi = x.astype(BF16)
    left = x - hi.astype(F32)
    mid = left.astype(BF16)
    lo = (left - mid.astype(F32)).astype(BF16)
    picked = (dot_tn(hi, hot) + dot_tn(mid, hot)) + dot_tn(lo, hot)
    mine = jnp.where(iota((128, ROWS), 0) == lane, picked, 0.0)
    mine = jnp.sum(mine, axis=0, keepdims=True) - pos_ref[...]
    for j in range(ROWS // 128):
        out_ref[j : j + 1, :] = mine[:, j * 128 : (j + 1) * 128]


def call(kernel, out_shape, *args, specs=None, scratch=()):
    single = not isinstance(out_shape, tuple)
    return pl.pallas_call(
        kernel,
        out_shape=out_shape,
        in_specs=specs or [VMEM] * len(args),
        out_specs=VMEM if single else (VMEM,) * len(out_shape),
        scratch_shapes=scratch,
        compiler_params=pltpu.CompilerParams(vmem_limit_bytes=24 * 1024 * 1024),
    )(*args)


def exchange(x):
    return lax.all_to_all(x, "dp", split_axis=0, concat_axis=0, tiled=True)


def steps(queries, candidates, bucket):
    b = bucket.reshape(1, ROWS)
    shape = jax.ShapeDtypeStruct
    hbm = pl.BlockSpec(memory_space=pltpu.HBM)
    rows = pltpu.VMEM((ROWS, WIDTH), BF16)
    packed, rank, pos = call(
        pack_kernel,
        (shape((PEERS, 48, HALF), BF16), shape((1, ROWS), jnp.int32), shape((1, ROWS), F32)),
        *[pltpu.with_memory_space_constraint(x, pltpu.HBM) for x in (b, queries, candidates)],
        specs=[hbm] * 3,
        scratch=[pltpu.VMEM((1, ROWS), jnp.int32), rows, rows] + [pltpu.SemaphoreType.DMA] * 3,
    )
    received = exchange(packed)
    own_c = call(candidates_kernel, shape((SLOTS, WIDTH), BF16), received)
    other_c = lax.ppermute(own_c, "rep", [(0, 1), (1, 0)])
    line = shape((1, SLOTS), F32)
    short = shape((1, 128), F32)
    low = pltpu.VMEM((SLOTS, HALF), BF16)
    own_q, total, gone, pos_sum = call(
        own_kernel, (shape((SLOTS, WIDTH), BF16), line, short, short),
        received, own_c, scratch=[low],
    )
    back, loss_sum, n = call(
        other_kernel, (shape((PEERS, 128), F32), short, short),
        own_q, own_c, other_c, total, gone, pos_sum,
        scratch=[low, pltpu.VMEM((2, SLOTS, COLS), F32), pltpu.VMEM((1, SLOTS), F32)],
    )
    other_sum = lax.ppermute(loss_sum, "rep", [(0, 1), (1, 0)])
    returned = exchange(back)
    query_loss = call(finish_kernel, shape((ROWS // 128, 128), F32), b, rank, pos, returned)
    mean = (loss_sum + other_sum) / jnp.maximum(n, 1.0)
    return (query_loss.reshape(ROWS), mean[0, 0:1])


def solution(mesh):
    in_specs = (P(("dp", "rep"), None), P(("dp", "rep"), None), P(("dp", "rep"), None))
    out_specs = (P(("dp", "rep")), P("dp"))
    return jax.shard_map(steps, mesh=mesh, in_specs=in_specs, out_specs=out_specs, check_vma=False)
```

```python
import math

import jax
import jax.numpy as jnp
from jax import lax
from jax.experimental import pallas as pl
from jax.experimental.pallas import tpu as pltpu
from jax.sharding import PartitionSpec as P


ROWS = 768
WIDTH = 256
HALF = 128
PEERS = 128
CAP = 12
SLOTS = PEERS * CAP
MAIN = PEERS * 8
REST = PEERS * 4
ABSENT = 64.0
NEG = -1e30
HUGE = 1e37
TINY = 1e-25
LN2 = math.log(2.0)
TO_LOG2 = 0.0625 / LN2

F32 = jnp.float32
BF16 = jnp.bfloat16
VMEM = pl.BlockSpec(memory_space=pltpu.VMEM)


def iota(shape, dim):
    return lax.broadcasted_iota(jnp.int32, shape, dim)


def dot_nn(a, b):
    return lax.dot_general(a, b, (((1,), (0,)), ((), ())), preferred_element_type=F32)


def dot_nt(a, b):
    return lax.dot_general(a, b, (((1,), (1,)), ((), ())), preferred_element_type=F32)


def dot_tn(a, b):
    return lax.dot_general(a, b, (((0,), (0,)), ((), ())), preferred_element_type=F32)


def ranks(b):
    blocks = ROWS // 128
    row = iota((128, 128), 0)
    hot = [(row == b[:, j * 128 : (j + 1) * 128]).astype(F32) for j in range(blocks)]
    stack = jnp.concatenate(hot, axis=0).astype(BF16)
    upper = (iota((128, 256), 0) < iota((128, 256), 1)).astype(F32).astype(BF16)
    both = dot_nn(stack, upper)
    before = jnp.zeros((128, 128), F32)
    rank = []
    for j in range(blocks):
        at = both[j * 128 : (j + 1) * 128]
        rank.append(jnp.sum(hot[j] * (at[:, :128] + before), axis=0, keepdims=True))
        before = before + at[:, 128:]
    return jnp.concatenate(rank, axis=1).astype(jnp.int32), before


def pack_kernel(
    b_hbm, q_hbm, c_hbm, out_ref, rank_ref, b_ref, q_ref, c_ref, b_sem, q_sem, c_sem
):
    load_b = pltpu.make_async_copy(b_hbm, b_ref, b_sem)
    load_c = pltpu.make_async_copy(c_hbm, c_ref, c_sem)
    load_q = pltpu.make_async_copy(q_hbm, q_ref, q_sem)
    load_b.start()
    load_c.start()
    load_q.start()
    load_b.wait()
    b = b_ref[...]
    rank, count = ranks(b)
    rank_ref[...] = rank
    count = count.astype(jnp.int32)
    main_key = jnp.where(rank < 8, b * 8 + rank, -1)
    rest_key = jnp.where(rank >= 8, b * 4 + rank - 8, -1)
    step = 64
    low = iota((step // 2, 8, WIDTH), 1) < 4
    slot = iota((step, 8, HALF), 1)
    lane = iota((step, 8, HALF), 2)
    load_c.wait()
    load_q.wait()
    q = q_ref[...]
    c = c_ref[...]
    for p0 in range(0, PEERS, step):
        main = (iota((step * 8, ROWS), 0) + p0 * 8 == main_key).astype(F32).astype(BF16)
        rest = (iota((step * 4, ROWS), 0) + p0 * 4 == rest_key).astype(F32).astype(BF16)
        both = jnp.concatenate([main, rest], axis=0)
        c_both = dot_nn(both, c)
        q_both = dot_nn(both, q)
        c_main = c_both[: step * 8].reshape(step, 8, WIDTH)
        q_main = q_both[: step * 8].reshape(step, 8, WIDTH)
        c_rest = c_both[step * 8 :].reshape(step // 2, 8, WIDTH)
        q_rest = q_both[step * 8 :].reshape(step // 2, 8, WIDTH)
        even = jnp.where(low, c_rest, pltpu.roll(q_rest, 4, 1))
        odd = jnp.where(low, pltpu.roll(c_rest, 4, 1), q_rest)
        mixed = jnp.stack([even, odd], axis=1).reshape(step, 8, WIDTH)
        have = jnp.broadcast_to(count[p0 : p0 + step][:, None, :], (step, 8, HALF))
        c_lo = jnp.where((lane == 0) & (slot >= have), ABSENT, c_main[:, :, :HALF])
        gone = (lane == 0) & (slot < 4) & (slot + 8 >= have)
        r_lo = jnp.where(gone, ABSENT, mixed[:, :, :HALF])
        out_ref[p0 : p0 + step, 0:16, :] = jnp.concatenate(
            [c_lo, c_main[:, :, HALF:]], axis=1
        ).astype(BF16)
        out_ref[p0 : p0 + step, 16:32, :] = jnp.concatenate(
            [r_lo, mixed[:, :, HALF:]], axis=1
        ).astype(BF16)
        out_ref[p0 : p0 + step, 32:48, :] = jnp.concatenate(
            [q_main[:, :, :HALF], q_main[:, :, HALF:]], axis=1
        ).astype(BF16)


def main_rows(in_ref, at, ref):
    tile = in_ref[:, at : at + 16, :].astype(F32)
    ref[0:MAIN, :HALF] = tile[:, :8, :].reshape(MAIN, HALF).astype(BF16)
    ref[0:MAIN, HALF:] = tile[:, 8:, :].reshape(MAIN, HALF).astype(BF16)


def rest_rows(in_ref, second, ref):
    tile = in_ref[:, 16:32, :].astype(F32)
    first = iota((PEERS // 2, 8, HALF), 1) < 4
    for half in range(2):
        part = tile[:, half * 8 : half * 8 + 8, :].reshape(PEERS // 2, 2, 8, HALF)
        even = part[:, 0]
        odd = part[:, 1]
        if second:
            rows = jnp.where(first, pltpu.roll(even, 4, 1), odd)
        else:
            rows = jnp.where(first, even, pltpu.roll(odd, 4, 1))
        ref[MAIN:SLOTS, half * HALF : (half + 1) * HALF] = rows.reshape(REST, HALF).astype(BF16)


def candidates_kernel(in_ref, c_ref):
    main_rows(in_ref, 0, c_ref)
    rest_rows(in_ref, False, c_ref)


COLS = 256
CHUNK = 256


def eights(x, op):
    return op(x.reshape(x.shape[0] // 8, 8, x.shape[1]), axis=0)


def zeroed(c_ref, lo_ref):
    gone = jnp.zeros((8, HALF), F32)
    for k in range(SLOTS // CHUNK):
        at = slice(k * CHUNK, (k + 1) * CHUNK)
        x = c_ref[at, :HALF].astype(F32)
        absent = x == ABSENT
        lo_ref[at, :] = jnp.where(absent, 0.0, x).astype(BF16)
        gone = gone + eights(jnp.where(absent, 1.0, 0.0), jnp.sum)
    return jnp.sum(jnp.sum(gone, axis=0, keepdims=True), axis=1, keepdims=True)


def sums(q, c_ref, lo_ref, chunk):
    total = jnp.zeros((8, COLS), F32)
    for k in range(SLOTS // chunk):
        at = slice(k * chunk, (k + 1) * chunk)
        rows = jnp.concatenate([lo_ref[at, :], c_ref[at, HALF:]], axis=1)
        total = total + eights(jnp.exp2(dot_nt(rows, q) * TO_LOG2), jnp.sum)
    return jnp.sum(total, axis=0, keepdims=True)


def exact(q_ref, c_refs, t_ref, lse_ref):
    steps = SLOTS // CHUNK

    def block(j, _):
        cols = pl.ds(pl.multiple_of(j * COLS, COLS), COLS)
        q = q_ref[cols, :]
        top = jnp.full((8, COLS), 2 * NEG, F32)
        for i, c_ref in enumerate(c_refs):

            def scores(k, top):
                at = pl.ds(pl.multiple_of(k * CHUNK, CHUNK), CHUNK)
                rows = c_ref[at, :]
                absent = rows[:, 0:1].astype(F32) == ABSENT
                t = dot_nt(rows, q) * TO_LOG2 + jnp.where(absent, NEG, 0.0)
                t_ref[i, at, :] = t
                return jnp.maximum(top, eights(t, jnp.max))

            top = lax.fori_loop(0, steps, scores, top)
        top = jnp.max(top, axis=0, keepdims=True)
        total = jnp.zeros((8, COLS), F32)
        for i in range(len(c_refs)):

            def add(k, total):
                at = pl.ds(pl.multiple_of(k * CHUNK, CHUNK), CHUNK)
                return total + eights(jnp.exp2(t_ref[i, at, :] - top), jnp.sum)

            total = lax.fori_loop(0, steps, add, total)
        lse_ref[:, cols] = top * LN2 + jnp.log(jnp.sum(total, axis=0, keepdims=True))
        return 0

    lax.fori_loop(0, SLOTS // COLS, block, 0)


def own_kernel(
    in_ref, c_ref, home_q_ref, home_c_ref, q_ref, total_ref, gone_ref, pos_ref, home_ref, lo_ref
):
    main_rows(in_ref, 32, q_ref)
    rest_rows(in_ref, True, q_ref)
    gone_ref[...] = jnp.broadcast_to(zeroed(c_ref, lo_ref), (1, 128))
    for j in range(SLOTS // COLS):
        cols = slice(j * COLS, (j + 1) * COLS)
        total_ref[:, cols] = sums(q_ref[cols, :], c_ref, lo_ref, 2 * CHUNK)
    pos = jnp.zeros((8, WIDTH), F32)
    for k in range(SLOTS // CHUNK):
        at = slice(k * CHUNK, (k + 1) * CHUNK)
        pos = pos + eights(q_ref[at, :].astype(F32) * c_ref[at, :].astype(F32), jnp.sum)
    pos = jnp.sum(pos, axis=0, keepdims=True)
    pos_ref[...] = pos[:, :HALF] + pos[:, HALF:]
    both = home_q_ref[...].astype(F32) * home_c_ref[...].astype(F32)
    hi = both.astype(BF16)
    lo = (both - hi.astype(F32)).astype(BF16)
    ones = jnp.ones((8, WIDTH), BF16)
    home_ref[...] = ((dot_nt(ones, hi) + dot_nt(ones, lo)) * 0.0625)[0:1]


def other_kernel(
    q_ref, own_ref, c_ref, total_ref, gone_ref, pos_ref, out_ref, sum_ref, n_ref, lo_ref, t_ref, lse_ref
):
    gone = zeroed(c_ref, lo_ref) + gone_ref[:, 0:1]
    count = 2 * SLOTS - gone
    most = least = None
    for j in range(SLOTS // COLS):
        cols = slice(j * COLS, (j + 1) * COLS)
        total = total_ref[:, cols] + sums(q_ref[cols, :], c_ref, lo_ref, CHUNK)
        present = total - gone
        lse_ref[:, cols] = jnp.log(jnp.maximum(present, TINY))
        most = total if j == 0 else jnp.maximum(most, total)
        least = present if j == 0 else jnp.minimum(least, present)
    most = jnp.max(most, axis=1, keepdims=True)
    least = jnp.min(least, axis=1, keepdims=True)
    redo = (count > 0) & ((most > HUGE) | (least < 0.25 * gone + TINY))

    @pl.when(jnp.max(jnp.where(redo, 1.0, 0.0)) > 0)
    def _():
        exact(q_ref, (own_ref, c_ref), t_ref, lse_ref)

    n = jnp.broadcast_to(count, (1, 128))
    n_ref[...] = n
    log_n = jnp.log(jnp.maximum(n, 1.0))
    lines = [lse_ref[:, t * 128 : (t + 1) * 128] - log_n for t in range(CAP)]
    loss = lines[0]
    for line in lines[1:]:
        loss = loss + line
    loss = jnp.sum(loss - pos_ref[...] * 0.0625, axis=1, keepdims=True)
    sum_ref[...] = jnp.broadcast_to(jnp.where(count > 0, loss, 0.0), (1, 128))
    lane = iota((1, 128), 1)
    for u in range(PEERS // 8):
        a = lines[u // 2]
        if u % 2:
            a = pltpu.roll(a, 64, 1)
        r = lines[8 + u // 4]
        shift = (64 - 32 * (u % 4)) % 128
        if shift:
            r = pltpu.roll(r, shift, 1)
        line = jnp.where(lane < 64, a, jnp.where(lane < 96, r, 0.0))
        out_ref[u * 8 : (u + 1) * 8, :] = jnp.broadcast_to(line, (8, 128))


def pick_kernel(b_ref, rank_ref, pos_ref, back_ref, out_ref):
    eighth = lax.axis_index("dp") & 7
    rank = rank_ref[...]
    lane = jnp.where(rank < 8, eighth * 8 + rank, 64 + eighth * 4 + rank - 8)
    hot = (iota((PEERS, ROWS), 0) == b_ref[...]).astype(F32).astype(BF16)
    x = back_ref[...]
    hi = x.astype(BF16)
    left = x - hi.astype(F32)
    mid = left.astype(BF16)
    lo = (left - mid.astype(F32)).astype(BF16)
    picked = (dot_tn(hi, hot) + dot_tn(mid, hot)) + dot_tn(lo, hot)
    mine = jnp.where(iota((128, ROWS), 0) == lane, picked, 0.0)
    mine = jnp.sum(mine, axis=0, keepdims=True) - pos_ref[...]
    for j in range(ROWS // 128):
        out_ref[j : j + 1, :] = mine[:, j * 128 : (j + 1) * 128]


def finish_kernel(mine_ref, sum_ref, other_ref, n_ref, out_ref, mean_ref):
    out_ref[...] = mine_ref[...]
    mean_ref[...] = (sum_ref[...] + other_ref[...]) / jnp.maximum(n_ref[...], 1.0)


def call(kernel, out_shape, *args, specs=None, scratch=()):
    single = not isinstance(out_shape, tuple)
    return pl.pallas_call(
        kernel,
        out_shape=out_shape,
        in_specs=specs or [VMEM] * len(args),
        out_specs=VMEM if single else (VMEM,) * len(out_shape),
        scratch_shapes=scratch,
        compiler_params=pltpu.CompilerParams(vmem_limit_bytes=24 * 1024 * 1024),
    )(*args)


def exchange(x):
    return lax.all_to_all(x, "dp", split_axis=0, concat_axis=0, tiled=True)


def steps(queries, candidates, bucket):
    b = bucket.reshape(1, ROWS)
    shape = jax.ShapeDtypeStruct
    hbm = pl.BlockSpec(memory_space=pltpu.HBM)
    rows = shape((ROWS, WIDTH), BF16)
    ints = shape((1, ROWS), jnp.int32)
    packed, rank, b_here, q_here, c_here = call(
        pack_kernel, (shape((PEERS, 48, HALF), BF16), ints, ints, rows, rows),
        *[pltpu.with_memory_space_constraint(x, pltpu.HBM) for x in (b, queries, candidates)],
        specs=[hbm] * 3,
        scratch=[pltpu.SemaphoreType.DMA] * 3,
    )
    received = exchange(packed)
    own_c = call(candidates_kernel, shape((SLOTS, WIDTH), BF16), received)
    other_c = lax.ppermute(own_c, "rep", [(0, 1), (1, 0)])
    line = shape((1, SLOTS), F32)
    short = shape((1, 128), F32)
    low = pltpu.VMEM((SLOTS, HALF), BF16)
    own_q, total, gone, pos_sum, pos = call(
        own_kernel,
        (shape((SLOTS, WIDTH), BF16), line, short, short, shape((1, ROWS), F32)),
        received, own_c, q_here, c_here, scratch=[low],
    )
    back, loss_sum, n = call(
        other_kernel, (shape((PEERS, 128), F32), short, short),
        own_q, own_c, other_c, total, gone, pos_sum,
        scratch=[low, pltpu.VMEM((2, SLOTS, COLS), F32), pltpu.VMEM((1, SLOTS), F32)],
    )
    other_sum = lax.ppermute(loss_sum, "rep", [(0, 1), (1, 0)])
    returned = exchange(back)
    mine = call(pick_kernel, shape((ROWS // 128, 128), F32), b_here, rank, pos, returned)
    query_loss, mean = call(
        finish_kernel, (shape((ROWS // 128, 128), F32), short),
        mine, loss_sum, other_sum, n,
    )
    return (query_loss.reshape(ROWS), mean[0, 0:1])


def solution(mesh):
    in_specs = (P(("dp", "rep"), None), P(("dp", "rep"), None), P(("dp", "rep"), None))
    out_specs = (P(("dp", "rep")), P("dp"))
    return jax.shard_map(steps, mesh=mesh, in_specs=in_specs, out_specs=out_specs, check_vma=False)
```

```python
import math

import jax
import jax.numpy as jnp
from jax import lax
from jax.experimental import pallas as pl
from jax.experimental.pallas import tpu as pltpu
from jax.sharding import PartitionSpec as P


ROWS = 768
WIDTH = 256
HALF = 128
PEERS = 128
CAP = 12
SLOTS = PEERS * CAP
MAIN = PEERS * 8
REST = PEERS * 4
ABSENT = 64.0
NEG = -1e30
HUGE = 1e37
TINY = 1e-25
LN2 = math.log(2.0)
TO_LOG2 = 0.0625 / LN2

F32 = jnp.float32
BF16 = jnp.bfloat16
VMEM = pl.BlockSpec(memory_space=pltpu.VMEM)


def iota(shape, dim):
    return lax.broadcasted_iota(jnp.int32, shape, dim)


def dot_nn(a, b):
    return lax.dot_general(a, b, (((1,), (0,)), ((), ())), preferred_element_type=F32)


def dot_nt(a, b):
    return lax.dot_general(a, b, (((1,), (1,)), ((), ())), preferred_element_type=F32)


def dot_tn(a, b):
    return lax.dot_general(a, b, (((0,), (0,)), ((), ())), preferred_element_type=F32)


def ranks(b):
    blocks = ROWS // 128
    row = iota((128, 128), 0)
    hot = [(row == b[:, j * 128 : (j + 1) * 128]).astype(F32) for j in range(blocks)]
    stack = jnp.concatenate(hot, axis=0).astype(BF16)
    upper = (iota((128, 256), 0) < iota((128, 256), 1)).astype(F32).astype(BF16)
    both = dot_nn(stack, upper)
    before = jnp.zeros((128, 128), F32)
    rank = []
    for j in range(blocks):
        at = both[j * 128 : (j + 1) * 128]
        rank.append(jnp.sum(hot[j] * (at[:, :128] + before), axis=0, keepdims=True))
        before = before + at[:, 128:]
    return jnp.concatenate(rank, axis=1).astype(jnp.int32), before


def pack_kernel(
    b_hbm, q_hbm, c_hbm, out_ref, rank_ref, b_ref, q_ref, c_ref, b_sem, q_sem, c_sem
):
    load_b = pltpu.make_async_copy(b_hbm, b_ref, b_sem)
    load_c = pltpu.make_async_copy(c_hbm, c_ref, c_sem)
    load_q = pltpu.make_async_copy(q_hbm, q_ref, q_sem)
    load_b.start()
    load_c.start()
    load_q.start()
    load_b.wait()
    b = b_ref[...]
    rank, count = ranks(b)
    rank_ref[...] = rank
    count = count.astype(jnp.int32)
    main_key = jnp.where(rank < 8, b * 8 + rank, -1)
    rest_key = jnp.where(rank >= 8, b * 4 + rank - 8, -1)
    step = 64
    low = iota((step // 2, 8, WIDTH), 1) < 4
    slot = iota((step, 8, HALF), 1)
    lane = iota((step, 8, HALF), 2)
    load_c.wait()
    c = c_ref[...]
    q = None
    for p0 in range(0, PEERS, step):
        main = (iota((step * 8, ROWS), 0) + p0 * 8 == main_key).astype(F32).astype(BF16)
        rest = (iota((step * 4, ROWS), 0) + p0 * 4 == rest_key).astype(F32).astype(BF16)
        both = jnp.concatenate([main, rest], axis=0)
        c_both = dot_nn(both, c)
        if q is None:
            load_q.wait()
            q = q_ref[...]
        q_both = dot_nn(both, q)
        c_main = c_both[: step * 8].reshape(step, 8, WIDTH)
        q_main = q_both[: step * 8].reshape(step, 8, WIDTH)
        c_rest = c_both[step * 8 :].reshape(step // 2, 8, WIDTH)
        q_rest = q_both[step * 8 :].reshape(step // 2, 8, WIDTH)
        even = jnp.where(low, c_rest, pltpu.roll(q_rest, 4, 1))
        odd = jnp.where(low, pltpu.roll(c_rest, 4, 1), q_rest)
        mixed = jnp.stack([even, odd], axis=1).reshape(step, 8, WIDTH)
        have = jnp.broadcast_to(count[p0 : p0 + step][:, None, :], (step, 8, HALF))
        c_lo = jnp.where((lane == 0) & (slot >= have), ABSENT, c_main[:, :, :HALF])
        gone = (lane == 0) & (slot < 4) & (slot + 8 >= have)
        r_lo = jnp.where(gone, ABSENT, mixed[:, :, :HALF])
        out_ref[p0 : p0 + step, 0:16, :] = jnp.concatenate(
            [c_lo, c_main[:, :, HALF:]], axis=1
        ).astype(BF16)
        out_ref[p0 : p0 + step, 16:32, :] = jnp.concatenate(
            [r_lo, mixed[:, :, HALF:]], axis=1
        ).astype(BF16)
        out_ref[p0 : p0 + step, 32:48, :] = jnp.concatenate(
            [q_main[:, :, :HALF], q_main[:, :, HALF:]], axis=1
        ).astype(BF16)


def main_rows(in_ref, at, ref):
    tile = in_ref[:, at : at + 16, :].astype(F32)
    ref[0:MAIN, :HALF] = tile[:, :8, :].reshape(MAIN, HALF).astype(BF16)
    ref[0:MAIN, HALF:] = tile[:, 8:, :].reshape(MAIN, HALF).astype(BF16)


def rest_rows(in_ref, second, ref):
    tile = in_ref[:, 16:32, :].astype(F32)
    first = iota((PEERS // 2, 8, HALF), 1) < 4
    for half in range(2):
        part = tile[:, half * 8 : half * 8 + 8, :].reshape(PEERS // 2, 2, 8, HALF)
        even = part[:, 0]
        odd = part[:, 1]
        if second:
            rows = jnp.where(first, pltpu.roll(even, 4, 1), odd)
        else:
            rows = jnp.where(first, even, pltpu.roll(odd, 4, 1))
        ref[MAIN:SLOTS, half * HALF : (half + 1) * HALF] = rows.reshape(REST, HALF).astype(BF16)


def candidates_kernel(in_ref, c_ref):
    main_rows(in_ref, 0, c_ref)
    rest_rows(in_ref, False, c_ref)


COLS = 256
CHUNK = 256


def eights(x, op):
    return op(x.reshape(x.shape[0] // 8, 8, x.shape[1]), axis=0)


def zeroed(c_ref, lo_ref):
    gone = jnp.zeros((8, HALF), F32)
    for k in range(SLOTS // CHUNK):
        at = slice(k * CHUNK, (k + 1) * CHUNK)
        x = c_ref[at, :HALF].astype(F32)
        absent = x == ABSENT
        lo_ref[at, :] = jnp.where(absent, 0.0, x).astype(BF16)
        gone = gone + eights(jnp.where(absent, 1.0, 0.0), jnp.sum)
    return jnp.sum(jnp.sum(gone, axis=0, keepdims=True), axis=1, keepdims=True)


def sums(q, c_ref, lo_ref, chunk):
    total = jnp.zeros((8, COLS), F32)
    for k in range(SLOTS // chunk):
        at = slice(k * chunk, (k + 1) * chunk)
        rows = jnp.concatenate([lo_ref[at, :], c_ref[at, HALF:]], axis=1)
        total = total + eights(jnp.exp2(dot_nt(rows, q) * TO_LOG2), jnp.sum)
    return jnp.sum(total, axis=0, keepdims=True)


def exact(q_ref, c_refs, t_ref, lse_ref):
    steps = SLOTS // CHUNK

    def block(j, _):
        cols = pl.ds(pl.multiple_of(j * COLS, COLS), COLS)
        q = q_ref[cols, :]
        top = jnp.full((8, COLS), 2 * NEG, F32)
        for i, c_ref in enumerate(c_refs):

            def scores(k, top):
                at = pl.ds(pl.multiple_of(k * CHUNK, CHUNK), CHUNK)
                rows = c_ref[at, :]
                absent = rows[:, 0:1].astype(F32) == ABSENT
                t = dot_nt(rows, q) * TO_LOG2 + jnp.where(absent, NEG, 0.0)
                t_ref[i, at, :] = t
                return jnp.maximum(top, eights(t, jnp.max))

            top = lax.fori_loop(0, steps, scores, top)
        top = jnp.max(top, axis=0, keepdims=True)
        total = jnp.zeros((8, COLS), F32)
        for i in range(len(c_refs)):

            def add(k, total):
                at = pl.ds(pl.multiple_of(k * CHUNK, CHUNK), CHUNK)
                return total + eights(jnp.exp2(t_ref[i, at, :] - top), jnp.sum)

            total = lax.fori_loop(0, steps, add, total)
        lse_ref[:, cols] = top * LN2 + jnp.log(jnp.sum(total, axis=0, keepdims=True))
        return 0

    lax.fori_loop(0, SLOTS // COLS, block, 0)


def own_kernel(
    in_ref, c_ref, home_q_ref, home_c_ref, b_ref, rank_ref,
    q_ref, total_ref, gone_ref, pos_ref, home_ref, hot_ref, lane_ref, lo_ref,
):
    main_rows(in_ref, 32, q_ref)
    rest_rows(in_ref, True, q_ref)
    gone_ref[...] = jnp.broadcast_to(zeroed(c_ref, lo_ref), (1, 128))
    for j in range(SLOTS // COLS):
        cols = slice(j * COLS, (j + 1) * COLS)
        total_ref[:, cols] = sums(q_ref[cols, :], c_ref, lo_ref, 2 * CHUNK)
    pos = jnp.zeros((8, WIDTH), F32)
    for k in range(SLOTS // CHUNK):
        at = slice(k * CHUNK, (k + 1) * CHUNK)
        pos = pos + eights(q_ref[at, :].astype(F32) * c_ref[at, :].astype(F32), jnp.sum)
    pos = jnp.sum(pos, axis=0, keepdims=True)
    pos_ref[...] = pos[:, :HALF] + pos[:, HALF:]
    both = home_q_ref[...].astype(F32) * home_c_ref[...].astype(F32)
    hi = both.astype(BF16)
    lo = (both - hi.astype(F32)).astype(BF16)
    ones = jnp.ones((8, WIDTH), BF16)
    home_ref[...] = ((dot_nt(ones, hi) + dot_nt(ones, lo)) * 0.0625)[0:1]
    eighth = lax.axis_index("dp") & 7
    rank = rank_ref[...]
    lane_ref[...] = jnp.where(rank < 8, eighth * 8 + rank, 64 + eighth * 4 + rank - 8)
    hot_ref[...] = (iota((PEERS, ROWS), 0) == b_ref[...]).astype(F32).astype(BF16)


def other_kernel(
    q_ref, own_ref, c_ref, total_ref, gone_ref, pos_ref, out_ref, sum_ref, n_ref, lo_ref, t_ref, lse_ref
):
    gone = zeroed(c_ref, lo_ref) + gone_ref[:, 0:1]
    count = 2 * SLOTS - gone
    most = least = None
    for j in range(SLOTS // COLS):
        cols = slice(j * COLS, (j + 1) * COLS)
        total = total_ref[:, cols] + sums(q_ref[cols, :], c_ref, lo_ref, CHUNK)
        present = total - gone
        lse_ref[:, cols] = jnp.log(jnp.maximum(present, TINY))
        most = total if j == 0 else jnp.maximum(most, total)
        least = present if j == 0 else jnp.minimum(least, present)
    most = jnp.max(most, axis=1, keepdims=True)
    least = jnp.min(least, axis=1, keepdims=True)
    redo = (count > 0) & ((most > HUGE) | (least < 0.25 * gone + TINY))

    @pl.when(jnp.max(jnp.where(redo, 1.0, 0.0)) > 0)
    def _():
        exact(q_ref, (own_ref, c_ref), t_ref, lse_ref)

    n = jnp.broadcast_to(count, (1, 128))
    n_ref[...] = n
    log_n = jnp.log(jnp.maximum(n, 1.0))
    lines = [lse_ref[:, t * 128 : (t + 1) * 128] - log_n for t in range(CAP)]
    loss = lines[0]
    for line in lines[1:]:
        loss = loss + line
    loss = jnp.sum(loss - pos_ref[...] * 0.0625, axis=1, keepdims=True)
    sum_ref[...] = jnp.broadcast_to(jnp.where(count > 0, loss, 0.0), (1, 128))
    lane = iota((1, 128), 1)
    for u in range(PEERS // 8):
        a = lines[u // 2]
        if u % 2:
            a = pltpu.roll(a, 64, 1)
        r = lines[8 + u // 4]
        shift = (64 - 32 * (u % 4)) % 128
        if shift:
            r = pltpu.roll(r, shift, 1)
        line = jnp.where(lane < 64, a, jnp.where(lane < 96, r, 0.0))
        out_ref[u * 8 : (u + 1) * 8, :] = jnp.broadcast_to(line, (8, 128))


def finish_kernel(
    hot_ref, lane_ref, pos_ref, sum_ref, other_ref, n_ref, back_ref, out_ref, mean_ref
):
    mean_ref[...] = (sum_ref[...] + other_ref[...]) / jnp.maximum(n_ref[...], 1.0)
    hot = hot_ref[...]
    x = back_ref[...]
    hi = x.astype(BF16)
    left = x - hi.astype(F32)
    mid = left.astype(BF16)
    lo = (left - mid.astype(F32)).astype(BF16)
    picked = (dot_tn(hi, hot) + dot_tn(mid, hot)) + dot_tn(lo, hot)
    mine = jnp.where(iota((128, ROWS), 0) == lane_ref[...], picked, 0.0)
    mine = jnp.sum(mine, axis=0, keepdims=True) - pos_ref[...]
    for j in range(ROWS // 128):
        out_ref[j : j + 1, :] = mine[:, j * 128 : (j + 1) * 128]


def call(kernel, out_shape, *args, specs=None, scratch=()):
    single = not isinstance(out_shape, tuple)
    return pl.pallas_call(
        kernel,
        out_shape=out_shape,
        in_specs=specs or [VMEM] * len(args),
        out_specs=VMEM if single else (VMEM,) * len(out_shape),
        scratch_shapes=scratch,
        compiler_params=pltpu.CompilerParams(vmem_limit_bytes=24 * 1024 * 1024),
    )(*args)


def exchange(x):
    return lax.all_to_all(x, "dp", split_axis=0, concat_axis=0, tiled=True)


def steps(queries, candidates, bucket):
    b = bucket.reshape(1, ROWS)
    shape = jax.ShapeDtypeStruct
    hbm = pl.BlockSpec(memory_space=pltpu.HBM)
    rows = shape((ROWS, WIDTH), BF16)
    ints = shape((1, ROWS), jnp.int32)
    packed, rank, b_here, q_here, c_here = call(
        pack_kernel, (shape((PEERS, 48, HALF), BF16), ints, ints, rows, rows),
        *[pltpu.with_memory_space_constraint(x, pltpu.HBM) for x in (b, queries, candidates)],
        specs=[hbm] * 3,
        scratch=[pltpu.SemaphoreType.DMA] * 3,
    )
    received = exchange(packed)
    own_c = call(candidates_kernel, shape((SLOTS, WIDTH), BF16), received)
    other_c = lax.ppermute(own_c, "rep", [(0, 1), (1, 0)])
    line = shape((1, SLOTS), F32)
    short = shape((1, 128), F32)
    low = pltpu.VMEM((SLOTS, HALF), BF16)
    own_q, total, gone, pos_sum, pos, hot, lane = call(
        own_kernel,
        (
            shape((SLOTS, WIDTH), BF16), line, short, short,
            shape((1, ROWS), F32), shape((PEERS, ROWS), BF16), ints,
        ),
        received, own_c, q_here, c_here, b_here, rank, scratch=[low],
    )
    back, loss_sum, n = call(
        other_kernel, (shape((PEERS, 128), F32), short, short),
        own_q, own_c, other_c, total, gone, pos_sum,
        scratch=[low, pltpu.VMEM((2, SLOTS, COLS), F32), pltpu.VMEM((1, SLOTS), F32)],
    )
    other_sum = lax.ppermute(loss_sum, "rep", [(0, 1), (1, 0)])
    returned = exchange(back)
    query_loss, mean = call(
        finish_kernel, (shape((ROWS // 128, 128), F32), short),
        hot, lane, pos, loss_sum, other_sum, n, returned,
    )
    return (query_loss.reshape(ROWS), mean[0, 0:1])


def solution(mesh):
    in_specs = (P(("dp", "rep"), None), P(("dp", "rep"), None), P(("dp", "rep"), None))
    out_specs = (P(("dp", "rep")), P("dp"))
    return jax.shard_map(steps, mesh=mesh, in_specs=in_specs, out_specs=out_specs, check_vma=False)
```
